32 devices in a mesh: ma: 4 (over y, x), freq: 8 (over z, core).
Axes of the slice: x: 2, y: 2, z: 4, core: 2. Of those that a mesh axis runs over, the one named last changes fastest.
Arguments:
- m_table: int32 [8], P('ma'), may hold values from 0 to 1023, as said below
- retained_modes: int32 [8], P('ma'), may hold values from 128 to 512, as said below
- cycle_ids: int32 [32], P('ma'), may hold values from 1 to 2047, as said below
- kl_coeffs: bfloat16 [8, 4, 512], P('ma', None, 'freq'), may hold values from -6 to 6
- kl_vectors: bfloat16 [8, 512, 32, 512], P('ma', 'freq'), may hold values from -0.375 to 0.375
- beam_matrix: bfloat16 [8, 32, 1024, 512], P('ma', 'freq'), may hold values from -0.00390625 to 0.00390625
Outputs:
- sky_maps: float32 [32, 2, 32, 2048], P('ma', None, 'freq')
The draws below stay inside these ranges and needn't reach their ends.
Inputs may be any that keep to these rules, and one draw needn't show every extreme that they name: `m_table`: all distinct; slots 2 q and 2 q + 1 hold two numbers that sum to 1023. `retained_modes`: some slot keeps all 512 modes. `cycle_ids`: all distinct.
All inputs are finite; a program needn't handle non-finite values.
Results may differ from the reference program's by a relative error of at most 0.01.
Values may be sent and summed in bfloat16 or wider, within the bound.
No kernel may reach another device: no remote copies, remote signals or barrier semaphores. Data moves between devices by JAX's collectives and lax.ppermute only.
A program may use at most 64 MiB of HBM per device.

```python
import math
import jax
import jax.numpy as jnp
from jax import lax

MMAX = 1024
NPHI = 2048
L = 1024
K = 512
NKL = 512
CH = 32
NSIDE = 512
MM = 8
R = 32


def paired_slots(key):
    chosen = jax.random.permutation(jax.random.fold_in(key, 3), MMAX // 2)[:MM // 2]
    has_zero = jnp.any(chosen == 0)
    place = jax.random.randint(jax.random.fold_in(key, 4), (), 0, MM // 2)
    forced = jnp.where(jnp.arange(MM // 2) == place, 0, chosen)
    chosen = jnp.where(has_zero, chosen, forced)
    paired = jnp.stack([chosen, MMAX - 1 - chosen], axis=1)
    return paired.reshape(MM).astype(jnp.int32)


def draw_m_table(key, part):
    return paired_slots(key)


def draw_retained_modes(key, part):
    counts = jax.random.randint(jax.random.fold_in(key, 1), (MM,), NKL // 4, NKL + 1)
    fullest = jax.random.randint(jax.random.fold_in(key, 2), (), 0, MM)
    return jnp.where(jnp.arange(MM) == fullest, NKL, counts).astype(jnp.int32)


def draw_cycle_ids(key, part):
    return (jax.random.permutation(key, 4 * NSIDE - 1)[:R] + 1).astype(jnp.int32)


def draw_kl_coeffs(key, part):
    m_values = paired_slots(key).astype(jnp.float32)
    exponent = 2.0 * m_values / float(MMAX - 1) - 1.7
    slot_scale = jnp.exp(math.log(10.0) * exponent)
    value_key = jax.random.fold_in(key, 11)
    base = jnp.clip(jax.random.normal(value_key, (MM, 4, NKL), jnp.float32), -3.0, 3.0)
    values = jnp.clip(base * slot_scale[:, None, None], -6.0, 6.0)
    return values.astype(jnp.bfloat16)


def spiked(entries, own_key, source, target, shards_of, factor):
    owner, partner = [(jnp.arange(entries.shape[position]) // (entries.shape[position] // shards_of)).reshape([-1 if axis == position else 1 for axis in range(entries.ndim)]) for position in (source, target)]
    chosen = jax.random.permutation(own_key, shards_of)[partner]
    strong = (owner == chosen) | (owner == (partner + shards_of // 2) % shards_of)
    return jnp.where(strong, factor * entries, entries)


def shard_levels(own_key, shape, pieces, least, top_value):
    def one(position, shards_of):
        draws = jax.random.uniform(jax.random.fold_in(jax.random.fold_in(own_key, 6), position), (shards_of,), jnp.float32, least / len(pieces), top_value / len(pieces))
        return jnp.repeat(jnp.exp(draws), shape[position] // shards_of).reshape((-1,) + (1,) * (len(shape) - position - 1))

    level = one(*pieces[0])
    for cut in pieces[1:]:
        level = level * one(*cut)
    return level


def gaussian(key, shape, deviation, bound, pieces=(), held_as=jnp.bfloat16):
    array = jax.random.normal(key, shape, jnp.float32) * deviation
    if len(pieces) > 0:
        array = shard_levels(key, shape, pieces, -0.22, 0.18) * array
    return jnp.clip(array, min=-bound, max=bound).astype(held_as)


def heavy_noise(rng, dims, spread, bound, pieces, heavy, kind=jnp.bfloat16):
    result = spread * jax.random.normal(rng, dims, jnp.float32)
    if pieces:
        result = result * shard_levels(rng, dims, pieces, -0.22, 0.18)
    return jnp.clip(spiked(result, jax.random.fold_in(rng, 3), *heavy), -bound, bound).astype(kind)


def setup_inputs(seed: int = 0) -> dict:
    streams_of = jax.random.split(jax.random.key(seed), 7)
    return {
        "m_table": draw_m_table(jax.random.fold_in(streams_of[6], 71), 0),
        "retained_modes": draw_retained_modes(jax.random.fold_in(streams_of[6], 71), 0),
        "cycle_ids": draw_cycle_ids(jax.random.fold_in(streams_of[6], 71), 0),
        "kl_coeffs": draw_kl_coeffs(jax.random.fold_in(streams_of[6], 71), 0),
        "kl_vectors": heavy_noise(streams_of[4], (MM, NKL, CH, K), NKL ** -0.5, 0.375, ((0, 4), (1, 8)), (1, 2, 8, 2.0)),
        "beam_matrix": gaussian(streams_of[5], (MM, CH, L, K), (4 * K * L) ** -0.5, 0.00390625, ((0, 4), (1, 8))),
    }


def cycle_angles(cycle_numbers):
    cycle_float = cycle_numbers.astype(jnp.float32)
    nside_float = float(NSIDE)
    from_pole = jnp.minimum(cycle_float, 4.0 * nside_float - cycle_float)
    hemisphere = jnp.where(cycle_float <= 2.0 * nside_float, 1.0, -1.0)
    polar_part = from_pole * from_pole / (3.0 * nside_float * nside_float)
    colatitude_cosine = 1.0 - polar_part
    polar_sin = from_pole / (math.sqrt(3.0) * nside_float) * jnp.sqrt(2.0 - polar_part)
    latitude_cosine = 4.0 / 3.0 - 2.0 * from_pole / (3.0 * nside_float)
    latitude_sine = jnp.sqrt(jnp.maximum(1.0 - latitude_cosine * latitude_cosine, 0.25))
    in_cap = from_pole < nside_float
    cos_theta = hemisphere * jnp.where(in_cap, colatitude_cosine, latitude_cosine)
    sin_theta = jnp.where(in_cap, polar_sin, latitude_sine)
    return (cos_theta, sin_theta)

def combine(before_part, after_part):
    upper_left = after_part[0] * before_part[0] + after_part[1] * before_part[2]
    upper_right = after_part[0] * before_part[1] + after_part[1] * before_part[3]
    lower_left = after_part[2] * before_part[0] + after_part[3] * before_part[2]
    lower_right = after_part[2] * before_part[1] + after_part[3] * before_part[3]
    weight = jnp.abs(upper_left) + jnp.abs(upper_right) + jnp.abs(lower_left) + jnp.abs(lower_right)
    return (upper_left / weight, upper_right / weight, lower_left / weight, lower_right / weight, before_part[4] + after_part[4] + jnp.log(weight))

def legendre_rows(m_value, cos_theta, sin_theta):
    m_float = m_value.astype(jnp.float32)
    offset_rows = jnp.arange(L, dtype=jnp.float32)[:, None]
    later_rows = jnp.maximum(offset_rows, 2.0)
    degree = m_float + later_rows
    factor = jnp.sqrt((4.0 * degree * degree - 1.0) / (later_rows * (degree + m_float)))
    damping = jnp.sqrt((later_rows - 1.0) * (degree - 1.0 + m_float) / (4.0 * (degree - 1.0) * (degree - 1.0) - 1.0))
    first_step = jnp.sqrt(2.0 * m_float + 3.0)
    grid_shape = (L, cos_theta.shape[0])
    upper_left = jnp.where(offset_rows >= 2.0, factor * cos_theta[None, :], jnp.where(offset_rows >= 1.0, first_step * cos_theta[None, :], 1.0))
    upper_left = jnp.broadcast_to(upper_left, grid_shape)
    upper_right = jnp.broadcast_to(jnp.where(offset_rows >= 2.0, -factor * damping, 0.0), grid_shape)
    lower_left = jnp.broadcast_to(jnp.where(offset_rows >= 1.0, 1.0, 0.0), grid_shape)
    lower_right = jnp.broadcast_to(jnp.where(offset_rows >= 1.0, 0.0, 1.0), grid_shape)
    weight = jnp.abs(upper_left) + jnp.abs(upper_right) + jnp.abs(lower_left) + jnp.abs(lower_right)
    elements = (upper_left / weight, upper_right / weight, lower_left / weight, lower_right / weight, jnp.log(weight))
    prefix = lax.associative_scan(combine, elements, axis=0)
    log_start = 0.5 * (jnp.log((2.0 * m_float + 1.0) / (4.0 * math.pi)) + lax.lgamma(m_float + 0.5) - 0.5 * math.log(math.pi) - lax.lgamma(m_float + 1.0))
    log_start = log_start + m_float * jnp.log(sin_theta)[None, :]
    return prefix[0] * jnp.exp(prefix[4] + log_start)

def synthesize(harmonic_slot, m_value, cos_theta, sin_theta):
    channels = harmonic_slot.shape[0]
    flat_rows = harmonic_slot.reshape(channels * 4, L)
    padded = jnp.concatenate([flat_rows, jnp.zeros_like(flat_rows)], axis=1)
    shifted = lax.dynamic_slice_in_dim(padded, m_value.astype(jnp.int32), L, 1)
    legendre = legendre_rows(m_value, cos_theta, sin_theta).astype(jnp.bfloat16)
    synth_maps = jnp.dot(shifted, legendre, preferred_element_type=jnp.float32)
    return synth_maps.astype(jnp.bfloat16).reshape(channels, 2, 2, cos_theta.shape[0])

def fourier_table(m_values):
    azimuth_angle = jnp.arange(NPHI, dtype=jnp.int32)
    phase_index = m_values.astype(jnp.int32)[:, None] * azimuth_angle[None, :] % NPHI
    angle_table = phase_index.astype(jnp.float32) * (2.0 * math.pi / NPHI)
    weight = jnp.where(m_values == 0, 1.0, 2.0)[:, None]
    return jnp.stack([weight * jnp.cos(angle_table), -weight * jnp.sin(angle_table)]).astype(jnp.bfloat16)

def reference(m_table, retained_modes, cycle_ids, kl_coeffs, kl_vectors, beam_matrix):
    cos_theta, sin_theta = cycle_angles(cycle_ids)

    def per_slot(slot_entry):
        coeffs, vectors, beam_position, m_value, kept_count = slot_entry
        mode_index = jnp.arange(NKL, dtype=jnp.int32)
        masked = jnp.where(mode_index[None, :] < kept_count, coeffs, jnp.zeros_like(coeffs))
        svd_flat = jnp.dot(masked, vectors.reshape(NKL, CH * K), preferred_element_type=jnp.float32)
        singular_coefficients = svd_flat.astype(jnp.bfloat16).reshape(4, CH, K)
        spherical_harmonic = jnp.einsum('exd,xgd->xeg', singular_coefficients.astype(jnp.float32), beam_position.astype(jnp.float32)).astype(jnp.bfloat16)
        return synthesize(spherical_harmonic, m_value, cos_theta, sin_theta)
    cycle_modes = lax.map(per_slot, (kl_coeffs, kl_vectors, beam_matrix, m_table, retained_modes))
    fourier = fourier_table(m_table)
    return jnp.einsum('mcsqr,qmt->rsct', cycle_modes.astype(jnp.float32), fourier.astype(jnp.float32))
```

```python
import functools
import math

import jax
import jax.numpy as jnp
from jax import lax
from jax.experimental import pallas as pl
from jax.experimental.pallas import tpu as pltpu
from jax.sharding import PartitionSpec as P

NPHI = 2048
L = 1024
NSIDE = 512
PARTS = 4
BLOCKS = 32
STEPS = L // BLOCKS
ROWS = 256
LANES = 128
GROUP = 16

f32 = jnp.float32
bf16 = jnp.bfloat16
VMEM = pl.BlockSpec(memory_space=pltpu.VMEM)
SMEM = pl.BlockSpec(memory_space=pltpu.SMEM)
HBM = pl.BlockSpec(memory_space=pl.ANY)
LIMIT = 48 * 1024 * 1024


def padded(width):
    return -(-width // LANES) * LANES


def iota(shape, axis):
    return lax.broadcasted_iota(jnp.int32, shape, axis)


def kl_kernel(offset_ref, kept_ref, coeff_ref, vectors_hbm, out_ref, held, spread, sems):
    slots, modes, channels, depth = vectors_hbm.shape
    group = min(GROUP, channels)
    pieces = out_ref.shape[0]
    share = channels // pieces

    def copy(s):
        return pltpu.make_async_copy(vectors_hbm.at[s], held.at[s], sems.at[s])

    for s in range(slots):
        copy(s).start()
    rows, columns = group * PARTS, modes * group
    expand = (iota((modes, columns), 1) // group == iota((modes, columns), 0)).astype(bf16)
    mode_index = offset_ref[0] + iota((PARTS, modes), 1)
    keep = iota((rows, columns), 1) % group == iota((rows, columns), 0) // PARTS
    for s in range(slots):
        masked = jnp.where(mode_index < kept_ref[s], coeff_ref[s].astype(f32), 0.0)
        tall = jnp.concatenate([masked] * group, axis=0).astype(bf16)
        wide = jnp.dot(tall, expand, preferred_element_type=f32)
        spread[s] = jnp.where(keep, wide, 0.0).astype(bf16)
    for s in range(slots):
        copy(s).wait()
        for g in range(channels // group):
            block = held[s, :, g * group : (g + 1) * group, :].reshape(columns, depth)
            sums = jnp.dot(spread[s], block, preferred_element_type=f32).astype(bf16)
            for i in range(group // share):
                out_ref[g * (group // share) + i, s] = sums[
                    i * share * PARTS : (i + 1) * share * PARTS
                ]


def kl_stage(offset, kept, coeffs, vectors, pieces):
    slots, modes, channels, depth = vectors.shape
    group = min(GROUP, channels)
    return pl.pallas_call(
        kl_kernel,
        out_shape=jax.ShapeDtypeStruct(
            (pieces, slots, channels // pieces * PARTS, depth), bf16
        ),
        in_specs=[SMEM, SMEM, VMEM, HBM],
        out_specs=VMEM,
        scratch_shapes=[
            pltpu.VMEM((slots, modes, channels, depth), bf16),
            pltpu.VMEM((slots, group * PARTS, modes * group), bf16),
            pltpu.SemaphoreType.DMA((slots,)),
        ],
        compiler_params=pltpu.CompilerParams(vmem_limit_bytes=LIMIT),
        name="kl_stage",
    )(offset, kept, coeffs, vectors)


def angles(cycle):
    n = float(NSIDE)
    p = jnp.minimum(cycle, 4.0 * n - cycle)
    t = p * p / (3.0 * n * n)
    cap_sin = p * (1.0 / (math.sqrt(3.0) * n)) * jnp.sqrt(2.0 - t)
    belt_cos = 4.0 / 3.0 - p * (2.0 / (3.0 * n))
    belt_sin = jnp.sqrt(jnp.maximum(1.0 - belt_cos * belt_cos, 0.25))
    cap = p < n
    cosine = jnp.where(cap, 1.0 - t, belt_cos)
    return jnp.where(cycle <= 2.0 * n, cosine, -cosine), jnp.where(cap, cap_sin, belt_sin)


def log2_start(m, sine):
    x = m + 4.25
    y = 1.0 / (x * x)
    series = 1.0 + y * (-1.0 / 64.0 + y * (21.0 / 8192.0 - y * (671.0 / 524288.0)))
    product = series * lax.rsqrt(x) * (1.0 / math.sqrt(math.pi))
    for k in range(1, 5):
        product = product * ((m + k) / (m + (k - 0.5)))
    scale = (2.0 * m + 1.0) * (1.0 / (4.0 * math.pi)) * product
    return (0.5 * jnp.log(scale) + m * jnp.log(sine)) * (1.0 / math.log(2.0))


def legendre_rows(m, cosine, sine, p_ref, q_ref, left, right, scale, table):
    width = m.shape[1]
    first = (iota((BLOCKS, width), 0) * STEPS).astype(f32)
    m_all = jnp.broadcast_to(m, (BLOCKS, width))
    c_all = jnp.broadcast_to(cosine, (BLOCKS, width))
    began = first > m_all
    p1 = jnp.where(began, 1.0, 0.0)
    p0 = jnp.zeros_like(p1)
    q1 = jnp.zeros_like(p1)
    q0 = p1

    def factors(l):
        over = (l - m_all) * (l + m_all)
        under = 4.0 * l * l - 1.0
        root = lax.rsqrt(jnp.maximum(over, 1.0) * jnp.maximum(under, 1.0))
        live = over > 0.0
        return jnp.where(live, under * root, 0.0), jnp.where(live, over * root, 0.0)

    _, last_inverse = factors(first - 1.0)
    last_inverse = jnp.where(began, last_inverse, 0.0)
    for i in range(STEPS):
        l = first + float(i)
        a, inverse = factors(l)
        above = l > m_all
        a = jnp.where(above, a, 0.0)
        rise = a * c_all
        fall = a * last_inverse
        p2 = rise * p1 - fall * p0
        q2 = rise * q1 - fall * q0
        p2 = jnp.where(l == m_all, 1.0, p2)
        p1, p0 = p2, p1
        q1, q0 = q2, q1
        last_inverse = jnp.where(above, inverse, 0.0)
        p_ref[i] = p2
        q_ref[i] = q2

    size = jnp.maximum(
        jnp.maximum(jnp.abs(p1), jnp.abs(p0)), jnp.maximum(jnp.abs(q1), jnp.abs(q0))
    )
    power = jnp.floor(jnp.log(jnp.maximum(size, 1.0)) * (1.0 / math.log(2.0)))
    power = jnp.where(power >= 20.0, power, 0.0)
    shrink = jnp.exp2(-power)
    p1, p0, q1, q0 = p1 * shrink, p0 * shrink, q1 * shrink, q0 * shrink

    start = log2_start(m, sine)
    start_power = jnp.floor(start)
    start_value = jnp.exp2(start - start_power)
    here = jnp.zeros((1, width), f32)
    before = jnp.zeros((1, width), f32)
    level = jnp.zeros((1, width), f32)
    for b in range(BLOCKS):
        enters = (m >= float(b * STEPS)) & (m < float((b + 1) * STEPS))
        here = jnp.where(enters, start_value, here)
        before = jnp.where(enters, 0.0, before)
        level = jnp.where(enters, start_power, level)
        left[b : b + 1] = here
        right[b : b + 1] = before
        scale[b : b + 1] = level
        here, before = (
            p1[b : b + 1] * here + q1[b : b + 1] * before,
            p0[b : b + 1] * here + q0[b : b + 1] * before,
        )
        large = jnp.maximum(jnp.abs(here), jnp.abs(before)) > 2.0**30
        factor = jnp.where(large, 2.0**-30, 1.0)
        here = here * factor
        before = before * factor
        level = level + power[b : b + 1] + jnp.where(large, 30.0, 0.0)

    half = jnp.exp2(jnp.maximum(scale[...] * 0.5, -120.0))
    from_left = left[...] * half
    from_right = right[...] * half
    for i in range(STEPS):
        rows = (from_left * p_ref[i] + from_right * q_ref[i]) * half
        for j in range(width // LANES):
            table[j, pl.ds(i, BLOCKS, stride=STEPS), :] = rows[:, j * LANES : (j + 1) * LANES]


def sine_quarter(z):
    x = z * (2.0 * math.pi)
    y = x * x
    return x * (
        1.0
        + y
        * (
            -1.0 / 6.0
            + y * (1.0 / 120.0 + y * (-1.0 / 5040.0 + y * (1.0 / 362880.0 - y / 39916800.0)))
        )
    )


def fourier_rows(m):
    turn = (m * iota((m.shape[0], NPHI), 1)) % NPHI
    z = turn.astype(f32) * (1.0 / NPHI)
    z = jnp.where(z >= 0.5, z - 1.0, z)
    size = jnp.abs(z)
    cosine = sine_quarter(0.25 - size)
    folded = sine_quarter(jnp.where(size > 0.25, 0.5 - size, size))
    sine = jnp.where(z < 0.0, -folded, folded)
    weight = jnp.where(m == 0, 1.0, 2.0)
    return weight * cosine, -weight * sine


def projection_kernel(
    m_ref, ids_ref, beam_hbm, folded_ref, fourier_ref,
    held, p_ref, q_ref, left, right, scale, table, turned, sums, woven, sems,
):
    slots, share, _, depth = beam_hbm.shape
    members, entries = ids_ref.shape
    cycles_each = entries - slots
    cycles = members * cycles_each
    pieces = L // ROWS

    def copy(s, t):
        return pltpu.make_async_copy(
            beam_hbm.at[s, :, pl.ds(t * ROWS, ROWS), :],
            held.at[s, :, pl.ds(t * ROWS, ROWS), :],
            sems.at[s, t],
        )

    def needed(s, t):
        return m_ref[s] < (t + 1) * ROWS

    for t in reversed(range(pieces)):
        for s in range(slots):
            pl.when(needed(s, t))(copy(s, t).start)

    width = padded(slots * cycles)
    lane = iota((1, width), 1)
    m = jnp.zeros((1, width), jnp.int32)
    for s in range(slots):
        m = jnp.where(lane // cycles == s, m_ref[s], m)
    cycle = jnp.zeros((1, width), jnp.int32)
    for a in range(members):
        for r in range(cycles_each):
            cycle = jnp.where(lane % cycles == a * cycles_each + r, ids_ref[a, slots + r], cycle)
    cosine, sine = angles(cycle.astype(f32))
    legendre_rows(m.astype(f32), cosine, sine, p_ref, q_ref, left, right, scale, table)
    for j in range(width // LANES):
        turned[j * LANES : (j + 1) * LANES] = table[j].T.astype(bf16)

    every = members * slots
    row = iota((every, 1), 0)
    m_every = jnp.zeros((every, 1), jnp.int32)
    for a in range(members):
        for s in range(slots):
            m_every = jnp.where(row == a * slots + s, ids_ref[a, s], m_every)
    real, imaginary = fourier_rows(m_every)
    fourier_ref[:every] = real.astype(bf16)
    fourier_ref[every:] = imaginary.astype(bf16)

    sums[...] = jnp.zeros_like(sums)
    for t in reversed(range(pieces)):
        for s in range(slots):

            @pl.when(needed(s, t))
            def _():
                copy(s, t).wait()
                lhs = turned[s * cycles : (s + 1) * cycles, t * ROWS : (t + 1) * ROWS]
                for c in range(share):
                    sums[s, c] += jnp.dot(
                        lhs, held[s, c, t * ROWS : (t + 1) * ROWS, :], preferred_element_type=f32
                    )

    for s in range(slots):
        for c in range(share):
            for j in range(depth // LANES):
                woven[s, j, pl.ds(c, cycles, stride=share), :] = sums[
                    s, c, :, j * LANES : (j + 1) * LANES
                ]
        for j in range(depth // LANES):
            folded_ref[s, :, j * LANES : (j + 1) * LANES] = woven[s, j].astype(bf16)


def projection(m_table, ids, beam):
    slots, share, _, depth = beam.shape
    members, entries = ids.shape
    cycles = members * (entries - slots)
    width = padded(slots * cycles)
    every = members * slots
    return pl.pallas_call(
        projection_kernel,
        out_shape=(
            jax.ShapeDtypeStruct((slots, cycles * share, depth), bf16),
            jax.ShapeDtypeStruct((2 * every, NPHI), bf16),
        ),
        in_specs=[SMEM, SMEM, HBM],
        out_specs=(VMEM, VMEM),
        scratch_shapes=[
            pltpu.VMEM((slots, share, L, depth), bf16),
            pltpu.VMEM((STEPS, BLOCKS, width), f32),
            pltpu.VMEM((STEPS, BLOCKS, width), f32),
            pltpu.VMEM((BLOCKS, width), f32),
            pltpu.VMEM((BLOCKS, width), f32),
            pltpu.VMEM((BLOCKS, width), f32),
            pltpu.VMEM((width // LANES, L, LANES), f32),
            pltpu.VMEM((width, L), bf16),
            pltpu.VMEM((slots, share, cycles, depth), f32),
            pltpu.VMEM((slots, depth // LANES, cycles * share, LANES), f32),
            pltpu.SemaphoreType.DMA((slots, L // ROWS)),
        ],
        compiler_params=pltpu.CompilerParams(vmem_limit_bytes=LIMIT),
        name="projection",
    )(m_table, ids, beam)


def cycle_kernel(parts_ref, folded_ref, out_ref):
    members, rows, columns = out_ref.shape
    slots = folded_ref.shape[0]
    per_slot = columns // slots
    share = per_slot // PARTS
    total = parts_ref[0].astype(f32)
    for i in range(1, parts_ref.shape[0]):
        total = total + parts_ref[i].astype(f32)
    singular = total.reshape(columns, total.shape[-1]).astype(bf16)
    shape = (members * rows, columns)
    values = jnp.zeros(shape, f32)
    for s in range(slots):
        product = lax.dot_general(
            folded_ref[s], singular, (((1,), (1,)), ((), ())),
            preferred_element_type=f32,
        )
        values = jnp.where(iota(shape, 1) // per_slot == s, product, values)
    same = iota(shape, 0) % share == (iota(shape, 1) // PARTS) % share
    values = jnp.where(same, values, 0.0).astype(bf16)
    for a in range(members):
        out_ref[a] = values[a * rows : (a + 1) * rows]


def cycle_values(parts, folded, members):
    _, slots, per_slot, _ = parts.shape
    rows = folded.shape[1] // members
    return pl.pallas_call(
        cycle_kernel,
        out_shape=jax.ShapeDtypeStruct((members, rows, slots * per_slot), bf16),
        in_specs=[VMEM, VMEM],
        out_specs=VMEM,
        compiler_params=pltpu.CompilerParams(vmem_limit_bytes=LIMIT),
        name="cycle_values",
    )(parts, folded)


def sky_kernel(values_ref, fourier_ref, out_ref):
    members, rows, columns = values_ref.shape
    every = fourier_ref.shape[0] // 2
    slots = every // members
    per_slot = columns // slots
    share = per_slot // PARTS
    shape = (columns, 2 * every)
    part = iota(shape, 0) % PARTS
    slot = iota(shape, 0) // per_slot
    target = iota(shape, 1)
    for d in range(2):
        folded = jnp.zeros((rows, 2 * every), f32)
        for a in range(members):
            choose = (part // 2 == d) & (target == (part % 2) * every + a * slots + slot)
            folded = folded + jnp.dot(
                values_ref[a], jnp.where(choose, 1.0, 0.0).astype(bf16), preferred_element_type=f32
            )
        maps = jnp.dot(folded.astype(bf16), fourier_ref[...], preferred_element_type=f32)
        out_ref[:, d] = maps.reshape(rows // share, share, NPHI)


def sky_maps(values, fourier, share):
    members, rows, columns = values.shape
    return pl.pallas_call(
        sky_kernel,
        out_shape=jax.ShapeDtypeStruct((rows // share, 2, share, NPHI), f32),
        in_specs=[VMEM, VMEM],
        out_specs=VMEM,
        compiler_params=pltpu.CompilerParams(vmem_limit_bytes=LIMIT),
        name="sky_maps",
    )(values, fourier)


def local(members, pieces, m_table, retained_modes, cycle_ids, kl_coeffs, kl_vectors, beam_matrix):
    ids = lax.all_gather(jnp.concatenate([m_table, cycle_ids]), "ma", axis=0, tiled=False)
    offset = (lax.axis_index("freq") * kl_coeffs.shape[2]).astype(jnp.int32).reshape(1)
    sums = kl_stage(offset, retained_modes, kl_coeffs, kl_vectors, pieces)
    parts = lax.all_to_all(sums, "freq", split_axis=0, concat_axis=0, tiled=True)
    folded, fourier = projection(m_table, ids, beam_matrix)
    values = cycle_values(parts, folded, members)
    values = lax.all_to_all(values, "ma", split_axis=0, concat_axis=0, tiled=True)
    return sky_maps(values, fourier, beam_matrix.shape[1])


def solution(mesh):
    placed = (
        P("ma"),
        P("ma"),
        P("ma"),
        P("ma", None, "freq"),
        P("ma", "freq", None, None),
        P("ma", "freq", None, None),
    )
    return jax.shard_map(
        functools.partial(local, mesh.shape["ma"], mesh.shape["freq"]),
        mesh=mesh,
        in_specs=placed,
        out_specs=P("ma", None, "freq", None),
        check_vma=False,
    )
```

```python
import functools
import math

import jax
import jax.numpy as jnp
from jax import lax
from jax.experimental import pallas as pl
from jax.experimental.pallas import tpu as pltpu
from jax.sharding import PartitionSpec as P


NPHI = 2048
L = 1024
NSIDE = 512
PARTS = 4
BLOCKS = 32
STEPS = L // BLOCKS
ROWS = 256
LANES = 128
GROUP = 16


f32 = jnp.float32
bf16 = jnp.bfloat16
VMEM = pl.BlockSpec(memory_space=pltpu.VMEM)
SMEM = pl.BlockSpec(memory_space=pltpu.SMEM)
HBM = pl.BlockSpec(memory_space=pltpu.HBM)
LIMIT = 16 * 1024 * 1024
SMALL = 2 * 1024 * 1024


def padded(width):
    return -(-width // LANES) * LANES


def iota(shape, axis):
    return lax.broadcasted_iota(jnp.int32, shape, axis)


def work(microseconds):
    return pl.CostEstimate(
        flops=int(microseconds * 1e9), transcendentals=0, bytes_accessed=4096
    )


def kl_kernel(kept_ref, coeff_ref, vectors_ref, keep_ref, send_ref, spread, ready):
    slots, modes, channels, depth = vectors_ref.shape
    group = min(GROUP, channels)
    pieces = keep_ref.shape[0] * 2
    share = channels // pieces
    place = lax.axis_index("freq")
    rows, columns = group * PARTS, modes * group
    expand = (iota((modes, columns), 1) // group == iota((modes, columns), 0)).astype(bf16)
    mode_index = place * modes + iota((PARTS, modes), 1)
    diagonal = iota((rows, columns), 1) % group == iota((rows, columns), 0) // PARTS
    for s in range(slots):
        masked = jnp.where(mode_index < kept_ref[s], coeff_ref[s].astype(f32), 0.0)
        tall = jnp.concatenate([masked] * group, axis=0).astype(bf16)
        wide = jnp.dot(tall, expand, preferred_element_type=f32)
        spread[s] = jnp.where(diagonal, wide, 0.0).astype(bf16)
    parity = place % 2
    for s in range(slots):
        for g in range(channels // group):
            block = vectors_ref[s, :, g * group : (g + 1) * group, :].reshape(columns, depth)
            sums = jnp.dot(spread[s], block, preferred_element_type=f32)
            for i in range(group // share):
                piece = g * (group // share) + i
                ready[(piece + parity) % 2, piece // 2, s] = sums[
                    i * share * PARTS : (i + 1) * share * PARTS
                ]
    keep_ref[...] = ready[0]
    send_ref[...] = ready[1].astype(bf16)


def kl_stage(kept, coeffs, vectors, pieces):
    slots, modes, channels, depth = vectors.shape
    group = min(GROUP, channels)
    shape = (pieces // 2, slots, channels // pieces * PARTS, depth)
    return pl.pallas_call(
        kl_kernel,
        out_shape=(jax.ShapeDtypeStruct(shape, f32), jax.ShapeDtypeStruct(shape, bf16)),
        in_specs=[SMEM, VMEM, VMEM],
        out_specs=(VMEM, VMEM),
        scratch_shapes=[
            pltpu.VMEM((slots, group * PARTS, modes * group), bf16),
            pltpu.VMEM((2, *shape), f32),
        ],
        compiler_params=pltpu.CompilerParams(vmem_limit_bytes=LIMIT),
        cost_estimate=work(2.0),
        name="kl_stage",
    )(kept, coeffs, vectors)


def fold_kernel(bit, held_ref, got_ref, keep_ref, send_ref):
    mine = (lax.axis_index("freq") // bit) % 2
    for i in range(keep_ref.shape[0]):
        keep_ref[i] = held_ref[2 * i + mine] + got_ref[2 * i + mine].astype(f32)
        other = 2 * i + 1 - mine
        send_ref[i] = (held_ref[other] + got_ref[other].astype(f32)).astype(bf16)


def fold_stage(bit, held, got):
    shape = (held.shape[0] // 2, *held.shape[1:])
    return pl.pallas_call(
        functools.partial(fold_kernel, bit),
        out_shape=(jax.ShapeDtypeStruct(shape, f32), jax.ShapeDtypeStruct(shape, bf16)),
        in_specs=[VMEM, VMEM],
        out_specs=(VMEM, VMEM),
        compiler_params=pltpu.CompilerParams(vmem_limit_bytes=LIMIT),
        name="fold_stage",
    )(held, got)


def stack_kernel(low_ref, high_ref, out_ref):
    rows = low_ref.shape[0]
    out_ref[:rows] = low_ref[...]
    out_ref[rows:] = high_ref[...]


def copy_kernel(in_ref, out_ref):
    out_ref[...] = in_ref[...]


def lead(value):
    return pl.pallas_call(
        copy_kernel,
        out_shape=jax.ShapeDtypeStruct(value.shape, value.dtype),
        in_specs=[VMEM],
        out_specs=VMEM,
        compiler_params=pltpu.CompilerParams(vmem_limit_bytes=SMALL),
        cost_estimate=work(4.0),
        name="lead",
    )(value)


def stack(low, high):
    return pl.pallas_call(
        stack_kernel,
        out_shape=jax.ShapeDtypeStruct((2 * low.shape[0], low.shape[1]), low.dtype),
        in_specs=[VMEM, VMEM],
        out_specs=VMEM,
        compiler_params=pltpu.CompilerParams(vmem_limit_bytes=SMALL),
        name="stack",
    )(low, high)


def angles(cycle):
    n = float(NSIDE)
    p = jnp.minimum(cycle, 4.0 * n - cycle)
    t = p * p / (3.0 * n * n)
    cap_sin = p * (1.0 / (math.sqrt(3.0) * n)) * jnp.sqrt(2.0 - t)
    belt_cos = 4.0 / 3.0 - p * (2.0 / (3.0 * n))
    belt_sin = jnp.sqrt(jnp.maximum(1.0 - belt_cos * belt_cos, 0.25))
    cap = p < n
    cosine = jnp.where(cap, 1.0 - t, belt_cos)
    return jnp.where(cycle <= 2.0 * n, cosine, -cosine), jnp.where(cap, cap_sin, belt_sin)


def log2_start(m, sine):
    x = m + 4.25
    y = 1.0 / (x * x)
    series = 1.0 + y * (-1.0 / 64.0 + y * (21.0 / 8192.0 - y * (671.0 / 524288.0)))
    product = series * lax.rsqrt(x) * (1.0 / math.sqrt(math.pi))
    for k in range(1, 5):
        product = product * ((m + k) / (m + (k - 0.5)))
    scale = (2.0 * m + 1.0) * (1.0 / (4.0 * math.pi)) * product
    return (0.5 * jnp.log(scale) + m * jnp.log(sine)) * (1.0 / math.log(2.0))


def legendre_rows(m, cosine, sine, p_ref, q_ref, left, right, scale, table):
    width = m.shape[1]
    first = (iota((BLOCKS, width), 0) * STEPS).astype(f32)
    m_all = jnp.broadcast_to(m, (BLOCKS, width))
    c_all = jnp.broadcast_to(cosine, (BLOCKS, width))
    began = first > m_all
    p1 = jnp.where(began, 1.0, 0.0)
    p0 = jnp.zeros_like(p1)
    q1 = jnp.zeros_like(p1)
    q0 = p1

    def factors(l):
        over = (l - m_all) * (l + m_all)
        under = 4.0 * l * l - 1.0
        root = lax.rsqrt(jnp.maximum(over, 1.0) * jnp.maximum(under, 1.0))
        live = over > 0.0
        return jnp.where(live, under * root, 0.0), jnp.where(live, over * root, 0.0)

    _, last_inverse = factors(first - 1.0)
    last_inverse = jnp.where(began, last_inverse, 0.0)
    for i in range(STEPS):
        l = first + float(i)
        a, inverse = factors(l)
        above = l > m_all
        a = jnp.where(above, a, 0.0)
        rise = a * c_all
        fall = a * last_inverse
        p2 = rise * p1 - fall * p0
        q2 = rise * q1 - fall * q0
        p2 = jnp.where(l == m_all, 1.0, p2)
        p1, p0 = p2, p1
        q1, q0 = q2, q1
        last_inverse = jnp.where(above, inverse, 0.0)
        p_ref[i] = p2
        q_ref[i] = q2

    size = jnp.maximum(
        jnp.maximum(jnp.abs(p1), jnp.abs(p0)), jnp.maximum(jnp.abs(q1), jnp.abs(q0))
    )
    power = jnp.floor(jnp.log(jnp.maximum(size, 1.0)) * (1.0 / math.log(2.0)))
    power = jnp.where(power >= 20.0, power, 0.0)
    shrink = jnp.exp2(-power)
    p1, p0, q1, q0 = p1 * shrink, p0 * shrink, q1 * shrink, q0 * shrink

    start = log2_start(m, sine)
    start_power = jnp.floor(start)
    start_value = jnp.exp2(start - start_power)
    here = jnp.zeros((1, width), f32)
    before = jnp.zeros((1, width), f32)
    level = jnp.zeros((1, width), f32)
    for b in range(BLOCKS):
        enters = (m >= float(b * STEPS)) & (m < float((b + 1) * STEPS))
        here = jnp.where(enters, start_value, here)
        before = jnp.where(enters, 0.0, before)
        level = jnp.where(enters, start_power, level)
        left[b : b + 1] = here
        right[b : b + 1] = before
        scale[b : b + 1] = level
        here, before = (
            p1[b : b + 1] * here + q1[b : b + 1] * before,
            p0[b : b + 1] * here + q0[b : b + 1] * before,
        )
        large = jnp.maximum(jnp.abs(here), jnp.abs(before)) > 2.0**30
        factor = jnp.where(large, 2.0**-30, 1.0)
        here = here * factor
        before = before * factor
        level = level + power[b : b + 1] + jnp.where(large, 30.0, 0.0)

    half = jnp.exp2(jnp.maximum(scale[...] * 0.5, -120.0))
    from_left = left[...] * half
    from_right = right[...] * half
    for i in range(STEPS):
        rows = (from_left * p_ref[i] + from_right * q_ref[i]) * half
        for j in range(width // LANES):
            table[j, pl.ds(i, BLOCKS, stride=STEPS), :] = rows[:, j * LANES : (j + 1) * LANES]


def sine_quarter(z):
    x = z * (2.0 * math.pi)
    y = x * x
    return x * (
        1.0
        + y
        * (
            -1.0 / 6.0
            + y * (1.0 / 120.0 + y * (-1.0 / 5040.0 + y * (1.0 / 362880.0 - y / 39916800.0)))
        )
    )


def fourier_rows(m):
    turn = (m * iota((m.shape[0], NPHI), 1)) % NPHI
    z = turn.astype(f32) * (1.0 / NPHI)
    z = jnp.where(z >= 0.5, z - 1.0, z)
    size = jnp.abs(z)
    cosine = sine_quarter(0.25 - size)
    folded = sine_quarter(jnp.where(size > 0.25, 0.5 - size, size))
    sine = jnp.where(z < 0.0, -folded, folded)
    weight = jnp.where(m == 0, 1.0, 2.0)
    return weight * cosine, -weight * sine


def legendre_kernel(
    slots, ids_ref, turned_ref, fourier_ref, p_ref, q_ref, left, right, scale, table
):
    members, entries = ids_ref.shape
    cycles_each = entries - slots
    cycles = members * cycles_each
    width = padded(slots * cycles)
    lane = iota((1, width), 1)
    m = jnp.zeros((1, width), jnp.int32)
    for s in range(slots):
        m = jnp.where(lane // cycles == s, ids_ref[0, s], m)
    cycle = jnp.zeros((1, width), jnp.int32)
    for a in range(members):
        for r in range(cycles_each):
            cycle = jnp.where(lane % cycles == a * cycles_each + r, ids_ref[a, slots + r], cycle)
    cosine, sine = angles(cycle.astype(f32))
    legendre_rows(m.astype(f32), cosine, sine, p_ref, q_ref, left, right, scale, table)
    for j in range(width // LANES):
        turned_ref[j * LANES : (j + 1) * LANES] = table[j].T.astype(bf16)

    every = members * slots
    row = iota((every, 1), 0)
    m_every = jnp.zeros((every, 1), jnp.int32)
    for a in range(members):
        for s in range(slots):
            m_every = jnp.where(row == a * slots + s, ids_ref[a, s], m_every)
    real, imaginary = fourier_rows(m_every)
    fourier_ref[:every] = real.astype(bf16)
    fourier_ref[every:] = imaginary.astype(bf16)


def legendre_stage(ids, slots):
    members, entries = ids.shape
    width = padded(slots * members * (entries - slots))
    return pl.pallas_call(
        functools.partial(legendre_kernel, slots),
        out_shape=(
            jax.ShapeDtypeStruct((width, L), bf16),
            jax.ShapeDtypeStruct((2 * members * slots, NPHI), bf16),
        ),
        in_specs=[SMEM],
        out_specs=(VMEM, VMEM),
        scratch_shapes=[
            pltpu.VMEM((STEPS, BLOCKS, width), f32),
            pltpu.VMEM((STEPS, BLOCKS, width), f32),
            pltpu.VMEM((BLOCKS, width), f32),
            pltpu.VMEM((BLOCKS, width), f32),
            pltpu.VMEM((BLOCKS, width), f32),
            pltpu.VMEM((width // LANES, L, LANES), f32),
        ],
        compiler_params=pltpu.CompilerParams(vmem_limit_bytes=LIMIT),
        cost_estimate=work(2.0),
        name="legendre_stage",
    )(ids)


def projection_kernel(ids_ref, turned_ref, beam_ref, folded_ref, sums, woven):
    slots, share, cycles, depth = sums.shape
    sums[...] = jnp.zeros_like(sums)
    for t in reversed(range(L // ROWS)):
        for s in range(slots):

            @pl.when(ids_ref[0, s] < (t + 1) * ROWS)
            def _():
                lhs = turned_ref[s * cycles : (s + 1) * cycles, t * ROWS : (t + 1) * ROWS]
                for c in range(share):
                    sums[s, c] += jnp.dot(
                        lhs,
                        beam_ref[s, c, t * ROWS : (t + 1) * ROWS, :],
                        preferred_element_type=f32,
                    )

    for s in range(slots):
        for c in range(share):
            for j in range(depth // LANES):
                woven[s, j, pl.ds(c, cycles, stride=share), :] = sums[
                    s, c, :, j * LANES : (j + 1) * LANES
                ]
        for j in range(depth // LANES):
            folded_ref[s, :, j * LANES : (j + 1) * LANES] = woven[s, j].astype(bf16)


def projection(ids, turned, beam, cycles):
    slots, share, _, depth = beam.shape
    return pl.pallas_call(
        projection_kernel,
        out_shape=jax.ShapeDtypeStruct((slots, cycles * share, depth), bf16),
        in_specs=[SMEM, VMEM, VMEM],
        out_specs=VMEM,
        scratch_shapes=[
            pltpu.VMEM((slots, share, cycles, depth), f32),
            pltpu.VMEM((slots, depth // LANES, cycles * share, LANES), f32),
        ],
        compiler_params=pltpu.CompilerParams(vmem_limit_bytes=LIMIT),
        cost_estimate=work(2.0),
        name="projection",
    )(ids, turned, beam)


def cycle_kernel(held_ref, got_ref, folded_ref, *out_refs):
    members = len(out_refs)
    rows, columns = out_refs[0].shape
    slots = folded_ref.shape[0]
    per_slot = columns // slots
    share = per_slot // PARTS
    total = held_ref[0] + got_ref[0].astype(f32)
    singular = total.reshape(columns, total.shape[-1]).astype(bf16)
    shape = (members * rows, columns)
    values = jnp.zeros(shape, f32)
    for s in range(slots):
        product = lax.dot_general(
            folded_ref[s], singular, (((1,), (1,)), ((), ())),
            preferred_element_type=f32,
        )
        values = jnp.where(iota(shape, 1) // per_slot == s, product, values)
    same = iota(shape, 0) % share == (iota(shape, 1) // PARTS) % share
    values = jnp.where(same, values, 0.0).astype(bf16)
    for a in range(members):
        out_refs[a][...] = values[a * rows : (a + 1) * rows]


def cycle_values(held, got, folded, members):
    _, slots, per_slot, _ = held.shape
    rows = folded.shape[1] // members
    return pl.pallas_call(
        cycle_kernel,
        out_shape=(jax.ShapeDtypeStruct((rows, slots * per_slot), bf16),) * members,
        in_specs=[VMEM, VMEM, VMEM],
        out_specs=(VMEM,) * members,
        compiler_params=pltpu.CompilerParams(vmem_limit_bytes=LIMIT),
        name="cycle_values",
    )(held, got, folded)


def sky_kernel(members, *refs):
    values_refs, (fourier_ref, out_ref) = refs[:members], refs[members:]
    rows, columns = values_refs[0].shape
    every = fourier_ref.shape[0] // 2
    slots = every // members
    per_slot = columns // slots
    share = per_slot // PARTS
    shape = (columns, 2 * every)
    part = iota(shape, 0) % PARTS
    slot = iota(shape, 0) // per_slot
    target = iota(shape, 1)
    for d in range(2):
        folded = jnp.zeros((rows, 2 * every), f32)
        for a in range(members):
            choose = (part // 2 == d) & (target == (part % 2) * every + a * slots + slot)
            folded = folded + jnp.dot(
                values_refs[a][...], jnp.where(choose, 1.0, 0.0).astype(bf16), preferred_element_type=f32
            )
        maps = jnp.dot(folded.astype(bf16), fourier_ref[...], preferred_element_type=f32)
        out_ref[:, d] = maps.reshape(rows // share, share, NPHI)


def sky_maps(values, fourier, share):
    members = len(values)
    rows = values[0].shape[0]
    return pl.pallas_call(
        functools.partial(sky_kernel, members),
        out_shape=jax.ShapeDtypeStruct((rows // share, 2, share, NPHI), f32),
        in_specs=[VMEM] * (members + 1),
        out_specs=VMEM,
        compiler_params=pltpu.CompilerParams(vmem_limit_bytes=LIMIT),
        name="sky_maps",
    )(*values, fourier)


def swap(value, axis, size, bit):
    return lax.ppermute(value, axis, [(k, k ^ bit) for k in range(size)])


def local(members, pieces, m_table, retained_modes, cycle_ids, kl_coeffs, kl_vectors, beam_matrix):
    slots, share = beam_matrix.shape[:2]
    ids = lead(jnp.concatenate([m_table, cycle_ids])[None])
    bit = 1
    while bit < members:
        far = swap(ids, "ma", members, bit)
        ids = stack(ids, far)
        bit *= 2
    held, send = kl_stage(retained_modes, kl_coeffs, kl_vectors, pieces)
    bit = 1
    while True:
        got = swap(send, "freq", pieces, bit)
        bit *= 2
        if bit == pieces:
            break
        held, send = fold_stage(bit, held, got)
    turned, fourier = legendre_stage(ids, slots)
    folded = projection(ids, turned, beam_matrix, members * cycle_ids.shape[0])
    values = cycle_values(held, got, folded, members)
    values = [swap(x, "ma", members, j) if j else x for j, x in enumerate(values)]
    return sky_maps(values, fourier, share)


def solution(mesh):
    placed = (
        P("ma"),
        P("ma"),
        P("ma"),
        P("ma", None, "freq"),
        P("ma", "freq", None, None),
        P("ma", "freq", None, None),
    )
    return jax.shard_map(
        functools.partial(local, mesh.shape["ma"], mesh.shape["freq"]),
        mesh=mesh,
        in_specs=placed,
        out_specs=P("ma", None, "freq", None),
        check_vma=False,
    )
```

```python
import functools
import math

import jax
import jax.numpy as jnp
from jax import lax
from jax.experimental import pallas as pl
from jax.experimental.pallas import tpu as pltpu
from jax.sharding import PartitionSpec as P


NPHI = 2048
L = 1024
NSIDE = 512
PARTS = 4
BLOCKS = 32
STEPS = L // BLOCKS
ROWS = 256
LANES = 128
CHUNKS = 4
GROUP = 16


f32 = jnp.float32
bf16 = jnp.bfloat16
VMEM = pl.BlockSpec(memory_space=pltpu.VMEM)
SMEM = pl.BlockSpec(memory_space=pltpu.SMEM)
HBM = pl.BlockSpec(memory_space=pltpu.HBM)
LIMIT = 16 * 1024 * 1024
SMALL = 2 * 1024 * 1024


def padded(width):
    return -(-width // LANES) * LANES


def iota(shape, axis):
    return lax.broadcasted_iota(jnp.int32, shape, axis)


def work(microseconds):
    return pl.CostEstimate(
        flops=int(microseconds * 1e9), transcendentals=0, bytes_accessed=4096
    )


def lead_kernel(in_ref, out_ref):
    out_ref[...] = in_ref[...]


def lead(ids):
    return pl.pallas_call(
        lead_kernel,
        out_shape=jax.ShapeDtypeStruct(ids.shape, ids.dtype),
        in_specs=[VMEM],
        out_specs=VMEM,
        compiler_params=pltpu.CompilerParams(vmem_limit_bytes=SMALL),
        cost_estimate=work(4.0),
        name="lead",
    )(ids)


def spread_kernel(kept_ref, coeff_ref, out_ref):
    slots, rows, columns = out_ref.shape
    modes = coeff_ref.shape[2]
    group = columns // modes
    place = lax.axis_index("freq")
    expand = (iota((modes, columns), 1) // group == iota((modes, columns), 0)).astype(bf16)
    mode_index = place * modes + iota((PARTS, modes), 1)
    tall = []
    for s in range(slots):
        masked = jnp.where(mode_index < kept_ref[s], coeff_ref[s].astype(f32), 0.0)
        tall += [masked] * group
    wide = jnp.dot(
        jnp.concatenate(tall, axis=0).astype(bf16), expand, preferred_element_type=f32
    )
    period = max(group, LANES)
    diagonal = iota((rows, period), 1) % group == iota((rows, period), 0) // PARTS
    for s in range(slots):
        for t in range(columns // period):
            lanes = slice(t * period, (t + 1) * period)
            piece = wide[s * rows : (s + 1) * rows, lanes]
            out_ref[s, :, lanes] = jnp.where(diagonal, piece, 0.0).astype(bf16)


def spread_stage(kept, coeffs, channels):
    slots, _, modes = coeffs.shape
    group = min(GROUP, channels)
    return pl.pallas_call(
        spread_kernel,
        out_shape=jax.ShapeDtypeStruct((slots, group * PARTS, modes * group), bf16),
        in_specs=[SMEM, VMEM],
        out_specs=VMEM,
        compiler_params=pltpu.CompilerParams(vmem_limit_bytes=SMALL),
        cost_estimate=work(1.0),
        name="spread_stage",
    )(kept, coeffs)


def kl_kernel(spread_ref, vectors_ref, keep_ref, send_ref, ready):
    slots, modes, channels, depth = vectors_ref.shape
    group = spread_ref.shape[1] // PARTS
    pieces = keep_ref.shape[0] * 2
    share = channels // pieces
    parity = lax.axis_index("freq") % 2
    for s in range(slots):
        for g in range(channels // group):
            block = vectors_ref[s, :, g * group : (g + 1) * group, :]
            sums = jnp.dot(
                spread_ref[s], block.reshape(modes * group, depth), preferred_element_type=f32
            )
            for i in range(group // share):
                piece = g * (group // share) + i
                ready[(piece + parity) % 2, piece // 2, s] = sums[
                    i * share * PARTS : (i + 1) * share * PARTS
                ]
    keep_ref[...] = ready[0]
    send_ref[...] = ready[1].astype(bf16)


def kl_stage(spread, vectors, pieces):
    slots, _, channels, depth = vectors.shape
    shape = (pieces // 2, slots, channels // pieces * PARTS, depth)
    return pl.pallas_call(
        kl_kernel,
        out_shape=(jax.ShapeDtypeStruct(shape, f32), jax.ShapeDtypeStruct(shape, bf16)),
        in_specs=[VMEM, VMEM],
        out_specs=(VMEM, VMEM),
        scratch_shapes=[pltpu.VMEM((2, *shape), f32)],
        compiler_params=pltpu.CompilerParams(vmem_limit_bytes=LIMIT),
        cost_estimate=work(2.0),
        name="kl_stage",
    )(spread, vectors)


def fold_kernel(bit, held_ref, got_ref, keep_ref, send_ref):
    mine = (lax.axis_index("freq") // bit) % 2
    for i in range(keep_ref.shape[0]):
        keep_ref[i] = held_ref[2 * i + mine] + got_ref[2 * i + mine].astype(f32)
        other = 2 * i + 1 - mine
        send_ref[i] = (held_ref[other] + got_ref[other].astype(f32)).astype(bf16)


def fold_stage(bit, held, got):
    shape = (held.shape[0] // 2, *held.shape[1:])
    return pl.pallas_call(
        functools.partial(fold_kernel, bit),
        out_shape=(jax.ShapeDtypeStruct(shape, f32), jax.ShapeDtypeStruct(shape, bf16)),
        in_specs=[VMEM, VMEM],
        out_specs=(VMEM, VMEM),
        compiler_params=pltpu.CompilerParams(vmem_limit_bytes=LIMIT),
        name="fold_stage",
    )(held, got)


def stack_kernel(low_ref, high_ref, out_ref):
    rows = low_ref.shape[0]
    out_ref[:rows] = low_ref[...]
    out_ref[rows:] = high_ref[...]


def stack(low, high):
    return pl.pallas_call(
        stack_kernel,
        out_shape=jax.ShapeDtypeStruct((2 * low.shape[0], low.shape[1]), low.dtype),
        in_specs=[VMEM, VMEM],
        out_specs=VMEM,
        compiler_params=pltpu.CompilerParams(vmem_limit_bytes=SMALL),
        name="stack",
    )(low, high)


def angles(cycle):
    n = float(NSIDE)
    p = jnp.minimum(cycle, 4.0 * n - cycle)
    t = p * p / (3.0 * n * n)
    cap_sin = p * (1.0 / (math.sqrt(3.0) * n)) * jnp.sqrt(2.0 - t)
    belt_cos = 4.0 / 3.0 - p * (2.0 / (3.0 * n))
    belt_sin = jnp.sqrt(jnp.maximum(1.0 - belt_cos * belt_cos, 0.25))
    cap = p < n
    cosine = jnp.where(cap, 1.0 - t, belt_cos)
    return jnp.where(cycle <= 2.0 * n, cosine, -cosine), jnp.where(cap, cap_sin, belt_sin)


def log2_start(m, sine):
    x = m + 4.25
    y = 1.0 / (x * x)
    series = 1.0 + y * (-1.0 / 64.0 + y * (21.0 / 8192.0 - y * (671.0 / 524288.0)))
    product = series * lax.rsqrt(x) * (1.0 / math.sqrt(math.pi))
    for k in range(1, 5):
        product = product * ((m + k) / (m + (k - 0.5)))
    scale = (2.0 * m + 1.0) * (1.0 / (4.0 * math.pi)) * product
    return (0.5 * jnp.log(scale) + m * jnp.log(sine)) * (1.0 / math.log(2.0))


def legendre_rows(m, cosine, sine, p_ref, q_ref, left, right, scale, table):
    width = m.shape[1]
    first = (iota((BLOCKS, width), 0) * STEPS).astype(f32)
    m_all = jnp.broadcast_to(m, (BLOCKS, width))
    c_all = jnp.broadcast_to(cosine, (BLOCKS, width))
    began = first > m_all
    p1 = jnp.where(began, 1.0, 0.0)
    p0 = jnp.zeros_like(p1)
    q1 = jnp.zeros_like(p1)
    q0 = p1

    def factors(l):
        over = (l - m_all) * (l + m_all)
        under = 4.0 * l * l - 1.0
        root = lax.rsqrt(jnp.maximum(over, 1.0) * jnp.maximum(under, 1.0))
        live = over > 0.0
        return jnp.where(live, under * root, 0.0), jnp.where(live, over * root, 0.0)

    _, last_inverse = factors(first - 1.0)
    last_inverse = jnp.where(began, last_inverse, 0.0)
    for i in range(STEPS):
        l = first + float(i)
        a, inverse = factors(l)
        above = l > m_all
        a = jnp.where(above, a, 0.0)
        rise = a * c_all
        fall = a * last_inverse
        p2 = rise * p1 - fall * p0
        q2 = rise * q1 - fall * q0
        p2 = jnp.where(l == m_all, 1.0, p2)
        p1, p0 = p2, p1
        q1, q0 = q2, q1
        last_inverse = jnp.where(above, inverse, 0.0)
        p_ref[i] = p2
        q_ref[i] = q2

    size = jnp.maximum(
        jnp.maximum(jnp.abs(p1), jnp.abs(p0)), jnp.maximum(jnp.abs(q1), jnp.abs(q0))
    )
    power = jnp.floor(jnp.log(jnp.maximum(size, 1.0)) * (1.0 / math.log(2.0)))
    power = jnp.where(power >= 20.0, power, 0.0)
    shrink = jnp.exp2(-power)
    p1, p0, q1, q0 = p1 * shrink, p0 * shrink, q1 * shrink, q0 * shrink

    start = log2_start(m, sine)
    start_power = jnp.floor(start)
    start_value = jnp.exp2(start - start_power)
    here = jnp.zeros((1, width), f32)
    before = jnp.zeros((1, width), f32)
    level = jnp.zeros((1, width), f32)
    for b in range(BLOCKS):
        enters = (m >= float(b * STEPS)) & (m < float((b + 1) * STEPS))
        here = jnp.where(enters, start_value, here)
        before = jnp.where(enters, 0.0, before)
        level = jnp.where(enters, start_power, level)
        left[b : b + 1] = here
        right[b : b + 1] = before
        scale[b : b + 1] = level
        here, before = (
            p1[b : b + 1] * here + q1[b : b + 1] * before,
            p0[b : b + 1] * here + q0[b : b + 1] * before,
        )
        large = jnp.maximum(jnp.abs(here), jnp.abs(before)) > 2.0**30
        factor = jnp.where(large, 2.0**-30, 1.0)
        here = here * factor
        before = before * factor
        level = level + power[b : b + 1] + jnp.where(large, 30.0, 0.0)

    half = jnp.exp2(jnp.maximum(scale[...] * 0.5, -120.0))
    from_left = left[...] * half
    from_right = right[...] * half
    for i in range(STEPS):
        rows = (from_left * p_ref[i] + from_right * q_ref[i]) * half
        for j in range(width // LANES):
            table[j, pl.ds(i, BLOCKS, stride=STEPS), :] = rows[:, j * LANES : (j + 1) * LANES]


def sine_quarter(z):
    x = z * (2.0 * math.pi)
    y = x * x
    return x * (
        1.0
        + y
        * (
            -1.0 / 6.0
            + y * (1.0 / 120.0 + y * (-1.0 / 5040.0 + y * (1.0 / 362880.0 - y / 39916800.0)))
        )
    )


def fourier_rows(m):
    turn = (m * iota((m.shape[0], NPHI), 1)) % NPHI
    z = turn.astype(f32) * (1.0 / NPHI)
    z = jnp.where(z >= 0.5, z - 1.0, z)
    size = jnp.abs(z)
    cosine = sine_quarter(0.25 - size)
    folded = sine_quarter(jnp.where(size > 0.25, 0.5 - size, size))
    sine = jnp.where(z < 0.0, -folded, folded)
    weight = jnp.where(m == 0, 1.0, 2.0)
    return weight * cosine, -weight * sine


def legendre_kernel(
    slots, per_slot, ids_ref, turned_ref, fourier_ref, p_ref, q_ref, left, right, scale, table
):
    members, entries = ids_ref.shape
    cycles_each = entries - slots
    cycles = members * cycles_each
    width = padded(slots * cycles)
    lane = iota((1, width), 1)
    m = jnp.zeros((1, width), jnp.int32)
    for s in range(slots):
        m = jnp.where(lane // cycles == s, ids_ref[0, s], m)
    cycle = jnp.zeros((1, width), jnp.int32)
    for a in range(members):
        for r in range(cycles_each):
            cycle = jnp.where(lane % cycles == a * cycles_each + r, ids_ref[a, slots + r], cycle)
    cosine, sine = angles(cycle.astype(f32))
    legendre_rows(m.astype(f32), cosine, sine, p_ref, q_ref, left, right, scale, table)
    for j in range(width // LANES):
        turned_ref[j * LANES : (j + 1) * LANES] = table[j].T.astype(bf16)

    every = members * slots
    row = iota((every, 1), 0)
    m_every = jnp.zeros((every, 1), jnp.int32)
    for a in range(members):
        for s in range(slots):
            m_every = jnp.where(row == a * slots + s, ids_ref[a, s], m_every)
    real, imaginary = fourier_rows(m_every)
    is_real = iota((per_slot, NPHI), 0) % 2 == 0
    for j in range(every):
        rows = jnp.where(is_real, real[j : j + 1], imaginary[j : j + 1])
        fourier_ref[j * per_slot : (j + 1) * per_slot] = rows.astype(bf16)


def legendre_stage(ids, slots, per_slot):
    members, entries = ids.shape
    width = padded(slots * members * (entries - slots))
    return pl.pallas_call(
        functools.partial(legendre_kernel, slots, per_slot),
        out_shape=(
            jax.ShapeDtypeStruct((width, L), bf16),
            jax.ShapeDtypeStruct((members * slots * per_slot, NPHI), bf16),
        ),
        in_specs=[SMEM],
        out_specs=(VMEM, VMEM),
        scratch_shapes=[
            pltpu.VMEM((STEPS, BLOCKS, width), f32),
            pltpu.VMEM((STEPS, BLOCKS, width), f32),
            pltpu.VMEM((BLOCKS, width), f32),
            pltpu.VMEM((BLOCKS, width), f32),
            pltpu.VMEM((BLOCKS, width), f32),
            pltpu.VMEM((width // LANES, L, LANES), f32),
        ],
        compiler_params=pltpu.CompilerParams(vmem_limit_bytes=LIMIT),
        cost_estimate=work(2.0),
        name="legendre_stage",
    )(ids)


def projection_kernel(ids_ref, turned_ref, beam_ref, folded_ref, sums, woven):
    slots, share, cycles, depth = sums.shape
    sums[...] = jnp.zeros_like(sums)
    for t in reversed(range(L // ROWS)):
        for s in range(slots):

            @pl.when(ids_ref[0, s] < (t + 1) * ROWS)
            def _():
                lhs = turned_ref[s * cycles : (s + 1) * cycles, t * ROWS : (t + 1) * ROWS]
                for c in range(share):
                    sums[s, c] += jnp.dot(
                        lhs,
                        beam_ref[s, c, t * ROWS : (t + 1) * ROWS, :],
                        preferred_element_type=f32,
                    )

    for s in range(slots):
        for c in range(share):
            for j in range(depth // LANES):
                woven[s, j, pl.ds(c, cycles, stride=share), :] = sums[
                    s, c, :, j * LANES : (j + 1) * LANES
                ]
        for j in range(depth // LANES):
            folded_ref[s, :, j * LANES : (j + 1) * LANES] = woven[s, j].astype(bf16)


def projection(ids, turned, beam, cycles):
    slots, share, _, depth = beam.shape
    return pl.pallas_call(
        projection_kernel,
        out_shape=jax.ShapeDtypeStruct((slots, cycles * share, depth), bf16),
        in_specs=[SMEM, VMEM, VMEM],
        out_specs=VMEM,
        scratch_shapes=[
            pltpu.VMEM((slots, share, cycles, depth), f32),
            pltpu.VMEM((slots, depth // LANES, cycles * share, LANES), f32),
        ],
        compiler_params=pltpu.CompilerParams(vmem_limit_bytes=LIMIT),
        cost_estimate=work(2.0),
        name="projection",
    )(ids, turned, beam)


def cycle_kernel(held_ref, got_ref, folded_ref, *out_refs):
    members = len(out_refs)
    rows, columns = out_refs[0].shape
    slots = folded_ref.shape[0]
    per_member = columns // members
    per_slot = per_member // slots
    share = per_slot // PARTS
    total = held_ref[0] + got_ref[0].astype(f32)
    singular = total.reshape(per_member, total.shape[-1]).astype(bf16)
    singular = jnp.concatenate([singular] * members, axis=0)
    shape = (members * rows, columns)
    row, column = iota(shape, 0), iota(shape, 1)
    slot = (column // per_slot) % slots
    values = jnp.zeros(shape, f32)
    for s in range(slots):
        product = lax.dot_general(
            folded_ref[s], singular, (((1,), (1,)), ((), ())), preferred_element_type=f32
        )
        values = jnp.where(slot == s, product, values)
    same = (row % share == (column // PARTS) % share) & (row // rows == column // per_member)
    values = jnp.where(same, values, 0.0).astype(bf16)
    for a in range(members):
        out_refs[a][...] = values[a * rows : (a + 1) * rows]


def cycle_values(held, got, folded, members):
    _, slots, per_slot, _ = held.shape
    rows = folded.shape[1] // members
    shape = jax.ShapeDtypeStruct((rows, members * slots * per_slot), bf16)
    return pl.pallas_call(
        cycle_kernel,
        out_shape=(shape,) * members,
        in_specs=[VMEM, VMEM, VMEM],
        out_specs=(VMEM,) * members,
        compiler_params=pltpu.CompilerParams(vmem_limit_bytes=LIMIT),
        name="cycle_values",
    )(held, got, folded)


def sky_kernel(members, *refs):
    values_refs, (fourier_ref, out_hbm, maps, sems) = refs[:members], refs[members:]
    rows, columns = values_refs[0].shape
    share = out_hbm.shape[2]
    values = values_refs[0][...].astype(f32)
    for ref in values_refs[1:]:
        values = values + ref[...].astype(f32)
    split = (iota((rows, columns), 1) % PARTS) // 2
    both = jnp.concatenate([jnp.where(split == d, values, 0.0) for d in range(2)], axis=0)
    both = both.astype(bf16)
    width = NPHI // CHUNKS
    copies = []
    for t in range(CHUNKS):
        part = slice(t * width, (t + 1) * width)
        result = jnp.dot(both, fourier_ref[:, part], preferred_element_type=f32)
        for d in range(2):
            maps[:, d, :, part] = result[d * rows : (d + 1) * rows].reshape(
                rows // share, share, width
            )
        copies.append(
            pltpu.make_async_copy(maps.at[:, :, :, part], out_hbm.at[:, :, :, part], sems.at[t])
        )
        copies[-1].start()
    for copy in copies:
        copy.wait()


def sky_maps(values, fourier, share):
    members = len(values)
    shape = (values[0].shape[0] // share, 2, share, NPHI)
    return pl.pallas_call(
        functools.partial(sky_kernel, members),
        out_shape=jax.ShapeDtypeStruct(shape, f32),
        in_specs=[VMEM] * (members + 1),
        out_specs=HBM,
        scratch_shapes=[pltpu.VMEM(shape, f32), pltpu.SemaphoreType.DMA((CHUNKS,))],
        compiler_params=pltpu.CompilerParams(vmem_limit_bytes=LIMIT),
        name="sky_maps",
    )(*values, fourier)


def swap(value, axis, size, bit):
    return lax.ppermute(value, axis, [(k, k ^ bit) for k in range(size)])


def local(members, pieces, m_table, retained_modes, cycle_ids, kl_coeffs, kl_vectors, beam_matrix):
    slots, share = beam_matrix.shape[:2]
    ids = lead(jnp.concatenate([m_table, cycle_ids])[None])
    bit = 1
    while bit < members:
        far = swap(ids, "ma", members, bit)
        ids = stack(ids, far)
        bit *= 2
    spread = spread_stage(retained_modes, kl_coeffs, kl_vectors.shape[2])
    held, send = kl_stage(spread, kl_vectors, pieces)
    bit = 1
    while True:
        got = swap(send, "freq", pieces, bit)
        bit *= 2
        if bit == pieces:
            break
        held, send = fold_stage(bit, held, got)
    turned, fourier = legendre_stage(ids, slots, share * PARTS)
    folded = projection(ids, turned, beam_matrix, members * cycle_ids.shape[0])
    values = cycle_values(held, got, folded, members)
    gathered = [values[0]]
    for j in range(1, members):
        gathered.append(swap(values[j], "ma", members, j))
    values = gathered
    return sky_maps(values, fourier, share)


def solution(mesh):
    placed = (
        P("ma"),
        P("ma"),
        P("ma"),
        P("ma", None, "freq"),
        P("ma", "freq", None, None),
        P("ma", "freq", None, None),
    )
    return jax.shard_map(
        functools.partial(local, mesh.shape["ma"], mesh.shape["freq"]),
        mesh=mesh,
        in_specs=placed,
        out_specs=P("ma", None, "freq", None),
        check_vma=False,
    )
```

```python
import functools
import math

import jax
import jax.numpy as jnp
from jax import lax
from jax.experimental import pallas as pl
from jax.experimental.pallas import tpu as pltpu
from jax.sharding import PartitionSpec as P


NPHI = 2048
L = 1024
NSIDE = 512
PARTS = 4
BLOCKS = 32
STEPS = L // BLOCKS + 1
ROWS = 256
LANES = 128
CHUNKS = 4
GROUP = 16


f32 = jnp.float32
bf16 = jnp.bfloat16
VMEM = pl.BlockSpec(memory_space=pltpu.VMEM)
SMEM = pl.BlockSpec(memory_space=pltpu.SMEM)
HBM = pl.BlockSpec(memory_space=pltpu.HBM)
LIMIT = 16 * 1024 * 1024
SMALL = 2 * 1024 * 1024


def padded(width):
    return -(-width // LANES) * LANES


def iota(shape, axis):
    return lax.broadcasted_iota(jnp.int32, shape, axis)


def work(microseconds):
    return pl.CostEstimate(
        flops=int(microseconds * 1e9), transcendentals=0, bytes_accessed=4096
    )


def lead_kernel(in_ref, out_ref):
    out_ref[...] = in_ref[...]


def lead(ids):
    return pl.pallas_call(
        lead_kernel,
        out_shape=jax.ShapeDtypeStruct(ids.shape, ids.dtype),
        in_specs=[VMEM],
        out_specs=VMEM,
        compiler_params=pltpu.CompilerParams(vmem_limit_bytes=SMALL),
        cost_estimate=work(4.0),
        name="lead",
    )(ids)


def spread_kernel(kept_ref, coeff_ref, out_ref):
    slots, rows, columns = out_ref.shape
    modes = coeff_ref.shape[2]
    group = columns // modes
    place = lax.axis_index("freq")
    expand = (iota((modes, columns), 1) // group == iota((modes, columns), 0)).astype(bf16)
    mode_index = place * modes + iota((PARTS, modes), 1)
    tall = []
    for s in range(slots):
        masked = jnp.where(mode_index < kept_ref[s], coeff_ref[s].astype(f32), 0.0)
        tall += [masked] * group
    wide = jnp.dot(
        jnp.concatenate(tall, axis=0).astype(bf16), expand, preferred_element_type=f32
    )
    period = max(group, LANES)
    diagonal = iota((rows, period), 1) % group == iota((rows, period), 0) // PARTS
    for s in range(slots):
        for t in range(columns // period):
            lanes = slice(t * period, (t + 1) * period)
            piece = wide[s * rows : (s + 1) * rows, lanes]
            out_ref[s, :, lanes] = jnp.where(diagonal, piece, 0.0).astype(bf16)


def spread_stage(kept, coeffs, channels):
    slots, _, modes = coeffs.shape
    group = min(GROUP, channels)
    return pl.pallas_call(
        spread_kernel,
        out_shape=jax.ShapeDtypeStruct((slots, group * PARTS, modes * group), bf16),
        in_specs=[SMEM, VMEM],
        out_specs=VMEM,
        compiler_params=pltpu.CompilerParams(vmem_limit_bytes=SMALL),
        cost_estimate=work(1.0),
        name="spread_stage",
    )(kept, coeffs)


def kl_kernel(spread_ref, vectors_ref, keep_ref, send_ref, ready):
    slots, modes, channels, depth = vectors_ref.shape
    group = spread_ref.shape[1] // PARTS
    pieces = keep_ref.shape[0] * 2
    share = channels // pieces
    parity = lax.axis_index("freq") % 2
    for s in range(slots):
        for g in range(channels // group):
            block = vectors_ref[s, :, g * group : (g + 1) * group, :]
            sums = jnp.dot(
                spread_ref[s], block.reshape(modes * group, depth), preferred_element_type=f32
            )
            for i in range(group // share):
                piece = g * (group // share) + i
                ready[(piece + parity) % 2, piece // 2, s] = sums[
                    i * share * PARTS : (i + 1) * share * PARTS
                ]
    keep_ref[...] = ready[0]
    send_ref[...] = ready[1].astype(bf16)


def kl_stage(spread, vectors, pieces):
    slots, _, channels, depth = vectors.shape
    shape = (pieces // 2, slots, channels // pieces * PARTS, depth)
    return pl.pallas_call(
        kl_kernel,
        out_shape=(jax.ShapeDtypeStruct(shape, f32), jax.ShapeDtypeStruct(shape, bf16)),
        in_specs=[VMEM, VMEM],
        out_specs=(VMEM, VMEM),
        scratch_shapes=[pltpu.VMEM((2, *shape), f32)],
        compiler_params=pltpu.CompilerParams(vmem_limit_bytes=LIMIT),
        cost_estimate=work(2.0),
        name="kl_stage",
    )(spread, vectors)


def fold_kernel(bit, held_ref, got_ref, keep_ref, send_ref):
    mine = (lax.axis_index("freq") // bit) % 2
    for i in range(keep_ref.shape[0]):
        keep_ref[i] = held_ref[2 * i + mine] + got_ref[2 * i + mine].astype(f32)
        other = 2 * i + 1 - mine
        send_ref[i] = (held_ref[other] + got_ref[other].astype(f32)).astype(bf16)


def fold_stage(bit, held, got):
    shape = (held.shape[0] // 2, *held.shape[1:])
    return pl.pallas_call(
        functools.partial(fold_kernel, bit),
        out_shape=(jax.ShapeDtypeStruct(shape, f32), jax.ShapeDtypeStruct(shape, bf16)),
        in_specs=[VMEM, VMEM],
        out_specs=(VMEM, VMEM),
        compiler_params=pltpu.CompilerParams(vmem_limit_bytes=LIMIT),
        name="fold_stage",
    )(held, got)


def stack_kernel(low_ref, high_ref, out_ref):
    rows = low_ref.shape[0]
    out_ref[:rows] = low_ref[...]
    out_ref[rows:] = high_ref[...]


def stack(low, high):
    return pl.pallas_call(
        stack_kernel,
        out_shape=jax.ShapeDtypeStruct((2 * low.shape[0], low.shape[1]), low.dtype),
        in_specs=[VMEM, VMEM],
        out_specs=VMEM,
        compiler_params=pltpu.CompilerParams(vmem_limit_bytes=SMALL),
        name="stack",
    )(low, high)


def angles(cycle):
    n = float(NSIDE)
    p = jnp.minimum(cycle, 4.0 * n - cycle)
    t = p * p / (3.0 * n * n)
    cap_sin = p * (1.0 / (math.sqrt(3.0) * n)) * jnp.sqrt(2.0 - t)
    belt_cos = 4.0 / 3.0 - p * (2.0 / (3.0 * n))
    belt_sin = jnp.sqrt(jnp.maximum(1.0 - belt_cos * belt_cos, 0.25))
    cap = p < n
    cosine = jnp.where(cap, 1.0 - t, belt_cos)
    return jnp.where(cycle <= 2.0 * n, cosine, -cosine), jnp.where(cap, cap_sin, belt_sin)


def log2_start(m, sine):
    x = m + 4.25
    y = 1.0 / (x * x)
    series = 1.0 + y * (-1.0 / 64.0 + y * (21.0 / 8192.0 - y * (671.0 / 524288.0)))
    product = series * lax.rsqrt(x) * (1.0 / math.sqrt(math.pi))
    for k in range(1, 5):
        product = product * ((m + k) / (m + (k - 0.5)))
    scale = (2.0 * m + 1.0) * (1.0 / (4.0 * math.pi)) * product
    return (0.5 * jnp.log(scale) + m * jnp.log(sine)) * (1.0 / math.log(2.0))


def legendre_rows(m, cosine, sine, p_ref, q_ref, left, right, scale, table):
    width = m.shape[1]
    first = (iota((BLOCKS, width), 0) * STEPS).astype(f32)
    m_all = jnp.broadcast_to(m, (BLOCKS, width))
    c_all = jnp.broadcast_to(cosine, (BLOCKS, width))
    began = first > m_all
    p1 = jnp.where(began, 1.0, 0.0)
    p0 = jnp.zeros_like(p1)
    q1 = jnp.zeros_like(p1)
    q0 = p1

    def factors(l):
        over = (l - m_all) * (l + m_all)
        under = 4.0 * l * l - 1.0
        root = lax.rsqrt(jnp.maximum(over, 1.0) * jnp.maximum(under, 1.0))
        live = over > 0.0
        return jnp.where(live, under * root, 0.0), jnp.where(live, over * root, 0.0)

    _, last_inverse = factors(first - 1.0)
    last_inverse = jnp.where(began, last_inverse, 0.0)
    for i in range(STEPS):
        l = first + float(i)
        a, inverse = factors(l)
        above = l > m_all
        a = jnp.where(above, a, 0.0)
        rise = a * c_all
        fall = a * last_inverse
        p2 = rise * p1 - fall * p0
        q2 = rise * q1 - fall * q0
        p2 = jnp.where(l == m_all, 1.0, p2)
        p1, p0 = p2, p1
        q1, q0 = q2, q1
        last_inverse = jnp.where(above, inverse, 0.0)
        p_ref[i] = p2
        q_ref[i] = q2

    size = jnp.maximum(
        jnp.maximum(jnp.abs(p1), jnp.abs(p0)), jnp.maximum(jnp.abs(q1), jnp.abs(q0))
    )
    power = jnp.floor(jnp.log(jnp.maximum(size, 1.0)) * (1.0 / math.log(2.0)))
    power = jnp.where(power >= 20.0, power, 0.0)
    shrink = jnp.exp2(-power)
    p1, p0, q1, q0 = p1 * shrink, p0 * shrink, q1 * shrink, q0 * shrink

    start = log2_start(m, sine)
    start_power = jnp.floor(start)
    start_value = jnp.exp2(start - start_power)
    here = jnp.zeros((1, width), f32)
    before = jnp.zeros((1, width), f32)
    level = jnp.zeros((1, width), f32)
    for b in range(BLOCKS):
        enters = (m >= float(b * STEPS)) & (m < float((b + 1) * STEPS))
        here = jnp.where(enters, start_value, here)
        before = jnp.where(enters, 0.0, before)
        level = jnp.where(enters, start_power, level)
        left[b : b + 1] = here
        right[b : b + 1] = before
        scale[b : b + 1] = level
        here, before = (
            p1[b : b + 1] * here + q1[b : b + 1] * before,
            p0[b : b + 1] * here + q0[b : b + 1] * before,
        )
        large = jnp.maximum(jnp.abs(here), jnp.abs(before)) > 2.0**30
        factor = jnp.where(large, 2.0**-30, 1.0)
        here = here * factor
        before = before * factor
        level = level + power[b : b + 1] + jnp.where(large, 30.0, 0.0)

    half = jnp.exp2(jnp.maximum(scale[...] * 0.5, -120.0))
    from_left = left[...] * half
    from_right = right[...] * half
    for i in range(STEPS):
        rows = (from_left * p_ref[i] + from_right * q_ref[i]) * half
        for j in range(width // LANES):
            table[j, pl.ds(i, BLOCKS, stride=STEPS), :] = rows[:, j * LANES : (j + 1) * LANES]


def sine_quarter(z):
    x = z * (2.0 * math.pi)
    y = x * x
    return x * (
        1.0
        + y
        * (
            -1.0 / 6.0
            + y * (1.0 / 120.0 + y * (-1.0 / 5040.0 + y * (1.0 / 362880.0 - y / 39916800.0)))
        )
    )


def fourier_rows(m):
    turn = (m * iota((m.shape[0], NPHI), 1)) % NPHI
    z = turn.astype(f32) * (1.0 / NPHI)
    z = jnp.where(z >= 0.5, z - 1.0, z)
    size = jnp.abs(z)
    cosine = sine_quarter(0.25 - size)
    folded = sine_quarter(jnp.where(size > 0.25, 0.5 - size, size))
    sine = jnp.where(z < 0.0, -folded, folded)
    weight = jnp.where(m == 0, 1.0, 2.0)
    return weight * cosine, -weight * sine


def legendre_kernel(
    slots, ids_ref, turned_ref, p_ref, q_ref, left, right, scale, table
):
    members, entries = ids_ref.shape
    cycles_each = entries - slots
    cycles = members * cycles_each
    width = padded(slots * cycles)
    lane = iota((1, width), 1)
    m = jnp.zeros((1, width), jnp.int32)
    for s in range(slots):
        m = jnp.where(lane // cycles == s, ids_ref[0, s], m)
    cycle = jnp.zeros((1, width), jnp.int32)
    for a in range(members):
        for r in range(cycles_each):
            cycle = jnp.where(lane % cycles == a * cycles_each + r, ids_ref[a, slots + r], cycle)
    cosine, sine = angles(cycle.astype(f32))
    legendre_rows(m.astype(f32), cosine, sine, p_ref, q_ref, left, right, scale, table)
    for j in range(width // LANES):
        turned_ref[j * LANES : (j + 1) * LANES] = table[j, :L].T.astype(bf16)


def fourier_kernel(slots, per_slot, ids_ref, fourier_ref):
    members = ids_ref.shape[0]
    every = members * slots
    row = iota((every, 1), 0)
    m_every = jnp.zeros((every, 1), jnp.int32)
    for a in range(members):
        for s in range(slots):
            m_every = jnp.where(row == a * slots + s, ids_ref[a, s], m_every)
    real, imaginary = fourier_rows(m_every)
    is_real = iota((per_slot, NPHI), 0) % 2 == 0
    for j in range(every):
        rows = jnp.where(is_real, real[j : j + 1], imaginary[j : j + 1])
        fourier_ref[j * per_slot : (j + 1) * per_slot] = rows.astype(bf16)


def fourier_stage(ids, slots, per_slot):
    rows = ids.shape[0] * slots * per_slot
    return pl.pallas_call(
        functools.partial(fourier_kernel, slots, per_slot),
        out_shape=jax.ShapeDtypeStruct((rows, NPHI), bf16),
        in_specs=[SMEM],
        out_specs=VMEM,
        compiler_params=pltpu.CompilerParams(vmem_limit_bytes=LIMIT),
        cost_estimate=work(0.5),
        name="fourier_stage",
    )(ids)


def legendre_stage(ids, slots):
    members, entries = ids.shape
    width = padded(slots * members * (entries - slots))
    return pl.pallas_call(
        functools.partial(legendre_kernel, slots),
        out_shape=jax.ShapeDtypeStruct((width, L), bf16),
        in_specs=[SMEM],
        out_specs=VMEM,
        scratch_shapes=[
            pltpu.VMEM((STEPS, BLOCKS, width), f32),
            pltpu.VMEM((STEPS, BLOCKS, width), f32),
            pltpu.VMEM((BLOCKS, width), f32),
            pltpu.VMEM((BLOCKS, width), f32),
            pltpu.VMEM((BLOCKS, width), f32),
            pltpu.VMEM((width // LANES, BLOCKS * STEPS, LANES), f32),
        ],
        compiler_params=pltpu.CompilerParams(vmem_limit_bytes=LIMIT),
        cost_estimate=work(2.0),
        name="legendre_stage",
    )(ids)


def projection_kernel(ids_ref, turned_ref, beam_ref, folded_ref, sums, woven):
    slots, share, _, depth = beam_ref.shape
    cycles = folded_ref.shape[1] // share
    last = L // ROWS
    for pair in range(0, slots, 2):
        low = ids_ref[0, pair] // ROWS
        counts = last - low
        for k in range(last + 1):
            first = (k < counts).astype(jnp.int32)
            slot = pair + 1 - first
            start = jnp.where(k < counts, low + k, last - 1 - low + k - counts)
            start = pl.multiple_of(start * ROWS, ROWS)
            lhs = turned_ref[
                pl.ds(pl.multiple_of(slot * cycles, cycles), cycles), pl.ds(start, ROWS)
            ]
            for c in range(share):
                sums[k, c] = jnp.dot(
                    lhs, beam_ref[slot, c, pl.ds(start, ROWS), :], preferred_element_type=f32
                )
        for s in range(2):
            for c in range(share):
                total = jnp.zeros((cycles, depth), f32)
                for k in range(last + 1):
                    mine = (k < counts) if s == 0 else (k >= counts)
                    total = total + jnp.where(mine, sums[k, c], 0.0)
                for j in range(depth // LANES):
                    woven[s, j, pl.ds(c, cycles, stride=share), :] = total[
                        :, j * LANES : (j + 1) * LANES
                    ]
            for j in range(depth // LANES):
                folded_ref[pair + s, :, j * LANES : (j + 1) * LANES] = woven[s, j].astype(bf16)


def projection(ids, turned, beam, cycles):
    slots, share, _, depth = beam.shape
    return pl.pallas_call(
        projection_kernel,
        out_shape=jax.ShapeDtypeStruct((slots, cycles * share, depth), bf16),
        in_specs=[SMEM, VMEM, VMEM],
        out_specs=VMEM,
        scratch_shapes=[
            pltpu.VMEM((L // ROWS + 1, share, cycles, depth), f32),
            pltpu.VMEM((2, depth // LANES, cycles * share, LANES), f32),
        ],
        compiler_params=pltpu.CompilerParams(vmem_limit_bytes=LIMIT),
        cost_estimate=work(2.0),
        name="projection",
    )(ids, turned, beam)


def cycle_kernel(held_ref, got_ref, folded_ref, *out_refs):
    members = len(out_refs)
    rows, columns = out_refs[0].shape
    slots = folded_ref.shape[0]
    per_member = columns // members
    per_slot = per_member // slots
    share = per_slot // PARTS
    total = held_ref[0] + got_ref[0].astype(f32)
    singular = total.reshape(per_member, total.shape[-1]).astype(bf16)
    singular = jnp.concatenate([singular] * members, axis=0)
    shape = (members * rows, columns)
    row, column = iota(shape, 0), iota(shape, 1)
    slot = (column // per_slot) % slots
    values = jnp.zeros(shape, f32)
    for s in range(slots):
        product = lax.dot_general(
            folded_ref[s], singular, (((1,), (1,)), ((), ())), preferred_element_type=f32
        )
        values = jnp.where(slot == s, product, values)
    same = (row % share == (column // PARTS) % share) & (row // rows == column // per_member)
    values = jnp.where(same, values, 0.0).astype(bf16)
    for a in range(members):
        out_refs[a][...] = values[a * rows : (a + 1) * rows]


def cycle_values(held, got, folded, members):
    _, slots, per_slot, _ = held.shape
    rows = folded.shape[1] // members
    shape = jax.ShapeDtypeStruct((rows, members * slots * per_slot), bf16)
    return pl.pallas_call(
        cycle_kernel,
        out_shape=(shape,) * members,
        in_specs=[VMEM, VMEM, VMEM],
        out_specs=(VMEM,) * members,
        compiler_params=pltpu.CompilerParams(vmem_limit_bytes=LIMIT),
        name="cycle_values",
    )(held, got, folded)


def sky_kernel(members, *refs):
    values_refs, (fourier_ref, out_hbm, maps, sems) = refs[:members], refs[members:]
    rows, columns = values_refs[0].shape
    share = out_hbm.shape[2]
    values = values_refs[0][...].astype(f32)
    for ref in values_refs[1:]:
        values = values + ref[...].astype(f32)
    split = (iota((rows, columns), 1) % PARTS) // 2
    both = jnp.concatenate([jnp.where(split == d, values, 0.0) for d in range(2)], axis=0)
    both = both.astype(bf16)
    width = NPHI // CHUNKS
    copies = []
    for t in range(CHUNKS):
        part = slice(t * width, (t + 1) * width)
        result = jnp.dot(both, fourier_ref[:, part], preferred_element_type=f32)
        for d in range(2):
            maps[:, d, :, part] = result[d * rows : (d + 1) * rows].reshape(
                rows // share, share, width
            )
        copies.append(
            pltpu.make_async_copy(maps.at[:, :, :, part], out_hbm.at[:, :, :, part], sems.at[t])
        )
        copies[-1].start()
    for copy in copies:
        copy.wait()


def sky_maps(values, fourier, share):
    members = len(values)
    shape = (values[0].shape[0] // share, 2, share, NPHI)
    return pl.pallas_call(
        functools.partial(sky_kernel, members),
        out_shape=jax.ShapeDtypeStruct(shape, f32),
        in_specs=[VMEM] * (members + 1),
        out_specs=HBM,
        scratch_shapes=[pltpu.VMEM(shape, f32), pltpu.SemaphoreType.DMA((CHUNKS,))],
        compiler_params=pltpu.CompilerParams(vmem_limit_bytes=LIMIT),
        name="sky_maps",
    )(*values, fourier)


def swap(value, axis, size, bit):
    return lax.ppermute(value, axis, [(k, k ^ bit) for k in range(size)])


def local(members, pieces, m_table, retained_modes, cycle_ids, kl_coeffs, kl_vectors, beam_matrix):
    slots, share = beam_matrix.shape[:2]
    ids = lead(jnp.concatenate([m_table, cycle_ids])[None])
    bit = 1
    while bit < members:
        far = swap(ids, "ma", members, bit)
        ids = stack(ids, far)
        bit *= 2
    spread = spread_stage(retained_modes, kl_coeffs, kl_vectors.shape[2])
    held, send = kl_stage(spread, kl_vectors, pieces)
    bit = 1
    while True:
        got = swap(send, "freq", pieces, bit)
        bit *= 2
        if bit == pieces:
            break
        held, send = fold_stage(bit, held, got)
    turned = legendre_stage(ids, slots)
    fourier = fourier_stage(ids, slots, share * PARTS)
    folded = projection(ids, turned, beam_matrix, members * cycle_ids.shape[0])
    values = cycle_values(held, got, folded, members)
    gathered = [values[0]]
    for j in range(1, members):
        gathered.append(swap(values[j], "ma", members, j))
    values = gathered
    return sky_maps(values, fourier, share)


def solution(mesh):
    placed = (
        P("ma"),
        P("ma"),
        P("ma"),
        P("ma", None, "freq"),
        P("ma", "freq", None, None),
        P("ma", "freq", None, None),
    )
    return jax.shard_map(
        functools.partial(local, mesh.shape["ma"], mesh.shape["freq"]),
        mesh=mesh,
        in_specs=placed,
        out_specs=P("ma", None, "freq", None),
        check_vma=False,
    )
```

```python
import functools
import math

import jax
import jax.numpy as jnp
from jax import lax
from jax.experimental import pallas as pl
from jax.experimental.pallas import tpu as pltpu
from jax.sharding import PartitionSpec as P


NPHI = 2048
L = 1024
NSIDE = 512
PARTS = 4
BLOCKS = 32
STEPS = L // BLOCKS + 1
ROWS = 256
LANES = 128
CHUNKS = 4
GROUP = 16


f32 = jnp.float32
bf16 = jnp.bfloat16
VMEM = pl.BlockSpec(memory_space=pltpu.VMEM)
SMEM = pl.BlockSpec(memory_space=pltpu.SMEM)
HBM = pl.BlockSpec(memory_space=pltpu.HBM)
LIMIT = 16 * 1024 * 1024
SMALL = 2 * 1024 * 1024


def padded(width):
    return -(-width // LANES) * LANES


def iota(shape, axis):
    return lax.broadcasted_iota(jnp.int32, shape, axis)


def work(microseconds):
    return pl.CostEstimate(
        flops=int(microseconds * 1e9), transcendentals=0, bytes_accessed=4096
    )


def lead_kernel(in_ref, out_ref):
    out_ref[...] = in_ref[...]


def lead(ids):
    return pl.pallas_call(
        lead_kernel,
        out_shape=jax.ShapeDtypeStruct(ids.shape, ids.dtype),
        in_specs=[VMEM],
        out_specs=VMEM,
        compiler_params=pltpu.CompilerParams(vmem_limit_bytes=SMALL),
        cost_estimate=work(3.0),
        name="lead",
    )(ids)


def spread_kernel(kept_ref, coeff_ref, out_ref):
    slots, rows, columns = out_ref.shape
    modes = coeff_ref.shape[2]
    group = columns // modes
    place = lax.axis_index("freq")
    expand = (iota((modes, columns), 1) // group == iota((modes, columns), 0)).astype(bf16)
    mode_index = place * modes + iota((PARTS, modes), 1)
    tall = []
    for s in range(slots):
        kept = mode_index < kept_ref[:, s : s + 1]
        tall += [jnp.where(kept, coeff_ref[s].astype(f32), 0.0)] * 2
    wide = jnp.dot(
        jnp.concatenate(tall, axis=0).astype(bf16), expand, preferred_element_type=f32
    )
    period = max(group, LANES)
    diagonal = iota((rows, period), 1) % group == iota((rows, period), 0) // PARTS
    for s in range(slots):
        for t in range(columns // period):
            lanes = slice(t * period, (t + 1) * period)
            piece = wide[s * 2 * PARTS : (s + 1) * 2 * PARTS, lanes]
            piece = jnp.concatenate([piece] * (rows // (2 * PARTS)), axis=0)
            out_ref[s, :, lanes] = jnp.where(diagonal, piece, 0.0).astype(bf16)


def spread_stage(kept, coeffs, channels):
    slots, _, modes = coeffs.shape
    group = min(GROUP, channels)
    return pl.pallas_call(
        spread_kernel,
        out_shape=jax.ShapeDtypeStruct((slots, group * PARTS, modes * group), bf16),
        in_specs=[VMEM, VMEM],
        out_specs=VMEM,
        compiler_params=pltpu.CompilerParams(vmem_limit_bytes=SMALL),
        cost_estimate=work(0.5),
        name="spread_stage",
    )(kept[None], coeffs)


def kl_kernel(spread_ref, vectors_ref, keep_ref, send_ref, ready):
    slots, modes, channels, depth = vectors_ref.shape
    group = spread_ref.shape[1] // PARTS
    pieces = keep_ref.shape[0] * 2
    share = channels // pieces
    parity = lax.axis_index("freq") % 2
    for s in range(slots):
        for g in range(channels // group):
            block = vectors_ref[s, :, g * group : (g + 1) * group, :]
            sums = jnp.dot(
                spread_ref[s], block.reshape(modes * group, depth), preferred_element_type=f32
            )
            for i in range(group // share):
                piece = g * (group // share) + i
                ready[(piece + parity) % 2, piece // 2, s] = sums[
                    i * share * PARTS : (i + 1) * share * PARTS
                ]
    keep_ref[...] = ready[0]
    send_ref[...] = ready[1].astype(bf16)


def kl_stage(spread, vectors, pieces):
    slots, _, channels, depth = vectors.shape
    shape = (pieces // 2, slots, channels // pieces * PARTS, depth)
    return pl.pallas_call(
        kl_kernel,
        out_shape=(jax.ShapeDtypeStruct(shape, f32), jax.ShapeDtypeStruct(shape, bf16)),
        in_specs=[VMEM, VMEM],
        out_specs=(VMEM, VMEM),
        scratch_shapes=[pltpu.VMEM((2, *shape), f32)],
        compiler_params=pltpu.CompilerParams(vmem_limit_bytes=LIMIT),
        cost_estimate=work(2.0),
        name="kl_stage",
    )(spread, vectors)


def gather_kernel(own_ref, first_ref, middle_ref, given_ref, out_ref):
    odd = lax.axis_index("freq") % 2 == 1
    first, given = first_ref[...], given_ref[...]
    out_ref[0:1] = own_ref[...]
    out_ref[1:2] = jnp.where(odd, given, first)
    out_ref[2:3] = middle_ref[...]
    out_ref[3:4] = jnp.where(odd, first, given)


def gather(*rows):
    return pl.pallas_call(
        gather_kernel,
        out_shape=jax.ShapeDtypeStruct((4, rows[0].shape[1]), rows[0].dtype),
        in_specs=[VMEM] * 4,
        out_specs=VMEM,
        compiler_params=pltpu.CompilerParams(vmem_limit_bytes=SMALL),
        name="gather",
    )(*rows)


def fold_kernel(bit, held_ref, got_ref, keep_ref, send_ref):
    mine = (lax.axis_index("freq") // bit) % 2
    for i in range(keep_ref.shape[0]):
        keep_ref[i] = held_ref[2 * i + mine] + got_ref[2 * i + mine].astype(f32)
        other = 2 * i + 1 - mine
        send_ref[i] = (held_ref[other] + got_ref[other].astype(f32)).astype(bf16)


def fold_stage(bit, held, got):
    shape = (held.shape[0] // 2, *held.shape[1:])
    return pl.pallas_call(
        functools.partial(fold_kernel, bit),
        out_shape=(jax.ShapeDtypeStruct(shape, f32), jax.ShapeDtypeStruct(shape, bf16)),
        in_specs=[VMEM, VMEM],
        out_specs=(VMEM, VMEM),
        compiler_params=pltpu.CompilerParams(vmem_limit_bytes=LIMIT),
        name="fold_stage",
    )(held, got)


def stack_kernel(low_ref, high_ref, out_ref):
    rows = low_ref.shape[0]
    out_ref[:rows] = low_ref[...]
    out_ref[rows:] = high_ref[...]


def stack(low, high):
    return pl.pallas_call(
        stack_kernel,
        out_shape=jax.ShapeDtypeStruct((2 * low.shape[0], low.shape[1]), low.dtype),
        in_specs=[VMEM, VMEM],
        out_specs=VMEM,
        compiler_params=pltpu.CompilerParams(vmem_limit_bytes=SMALL),
        name="stack",
    )(low, high)


def angles(cycle):
    n = float(NSIDE)
    p = jnp.minimum(cycle, 4.0 * n - cycle)
    t = p * p / (3.0 * n * n)
    cap_sin = p * (1.0 / (math.sqrt(3.0) * n)) * jnp.sqrt(2.0 - t)
    belt_cos = 4.0 / 3.0 - p * (2.0 / (3.0 * n))
    belt_sin = jnp.sqrt(jnp.maximum(1.0 - belt_cos * belt_cos, 0.25))
    cap = p < n
    cosine = jnp.where(cap, 1.0 - t, belt_cos)
    return jnp.where(cycle <= 2.0 * n, cosine, -cosine), jnp.where(cap, cap_sin, belt_sin)


def log2_start(m, sine):
    x = m + 4.25
    y = 1.0 / (x * x)
    series = 1.0 + y * (-1.0 / 64.0 + y * (21.0 / 8192.0 - y * (671.0 / 524288.0)))
    product = series * lax.rsqrt(x) * (1.0 / math.sqrt(math.pi))
    for k in range(1, 5):
        product = product * ((m + k) / (m + (k - 0.5)))
    scale = (2.0 * m + 1.0) * (1.0 / (4.0 * math.pi)) * product
    return (0.5 * jnp.log(scale) + m * jnp.log(sine)) * (1.0 / math.log(2.0))


def legendre_rows(m, cosine, sine, p_ref, q_ref, left, right, scale, table):
    width = m.shape[1]
    first = (iota((BLOCKS, width), 0) * STEPS).astype(f32)
    m_all = jnp.broadcast_to(m, (BLOCKS, width))
    c_all = jnp.broadcast_to(cosine, (BLOCKS, width))
    began = first > m_all
    p1 = jnp.where(began, 1.0, 0.0)
    p0 = jnp.zeros_like(p1)
    q1 = jnp.zeros_like(p1)
    q0 = p1

    def factors(l):
        over = (l - m_all) * (l + m_all)
        under = 4.0 * l * l - 1.0
        root = lax.rsqrt(jnp.maximum(over, 1.0) * jnp.maximum(under, 1.0))
        live = over > 0.0
        return jnp.where(live, under * root, 0.0), jnp.where(live, over * root, 0.0)

    _, last_inverse = factors(first - 1.0)
    last_inverse = jnp.where(began, last_inverse, 0.0)
    for i in range(STEPS):
        l = first + float(i)
        a, inverse = factors(l)
        above = l > m_all
        a = jnp.where(above, a, 0.0)
        rise = a * c_all
        fall = a * last_inverse
        p2 = rise * p1 - fall * p0
        q2 = rise * q1 - fall * q0
        p2 = jnp.where(l == m_all, 1.0, p2)
        p1, p0 = p2, p1
        q1, q0 = q2, q1
        last_inverse = jnp.where(above, inverse, 0.0)
        p_ref[i] = p2
        q_ref[i] = q2

    size = jnp.maximum(
        jnp.maximum(jnp.abs(p1), jnp.abs(p0)), jnp.maximum(jnp.abs(q1), jnp.abs(q0))
    )
    power = jnp.floor(jnp.log(jnp.maximum(size, 1.0)) * (1.0 / math.log(2.0)))
    power = jnp.where(power >= 20.0, power, 0.0)
    shrink = jnp.exp2(-power)
    p1, p0, q1, q0 = p1 * shrink, p0 * shrink, q1 * shrink, q0 * shrink

    start = log2_start(m, sine)
    start_power = jnp.floor(start)
    start_value = jnp.exp2(start - start_power)
    here = jnp.zeros((1, width), f32)
    before = jnp.zeros((1, width), f32)
    level = jnp.zeros((1, width), f32)
    for b in range(BLOCKS):
        enters = (m >= float(b * STEPS)) & (m < float((b + 1) * STEPS))
        here = jnp.where(enters, start_value, here)
        before = jnp.where(enters, 0.0, before)
        level = jnp.where(enters, start_power, level)
        left[b : b + 1] = here
        right[b : b + 1] = before
        scale[b : b + 1] = level
        here, before = (
            p1[b : b + 1] * here + q1[b : b + 1] * before,
            p0[b : b + 1] * here + q0[b : b + 1] * before,
        )
        large = jnp.maximum(jnp.abs(here), jnp.abs(before)) > 2.0**30
        factor = jnp.where(large, 2.0**-30, 1.0)
        here = here * factor
        before = before * factor
        level = level + power[b : b + 1] + jnp.where(large, 30.0, 0.0)

    half = jnp.exp2(jnp.maximum(scale[...] * 0.5, -120.0))
    from_left = left[...] * half
    from_right = right[...] * half
    for i in range(STEPS):
        rows = (from_left * p_ref[i] + from_right * q_ref[i]) * half
        for j in range(width // LANES):
            table[j, pl.ds(i, BLOCKS, stride=STEPS), :] = rows[:, j * LANES : (j + 1) * LANES]


def sine_quarter(z):
    x = z * (2.0 * math.pi)
    y = x * x
    return x * (
        1.0
        + y
        * (
            -1.0 / 6.0
            + y * (1.0 / 120.0 + y * (-1.0 / 5040.0 + y * (1.0 / 362880.0 - y / 39916800.0)))
        )
    )


def fourier_rows(m):
    turn = (m * iota((m.shape[0], NPHI), 1)) % NPHI
    z = turn.astype(f32) * (1.0 / NPHI)
    z = jnp.where(z >= 0.5, z - 1.0, z)
    size = jnp.abs(z)
    cosine = sine_quarter(0.25 - size)
    folded = sine_quarter(jnp.where(size > 0.25, 0.5 - size, size))
    sine = jnp.where(z < 0.0, -folded, folded)
    weight = jnp.where(m == 0, 1.0, 2.0)
    return weight * cosine, -weight * sine


def legendre_kernel(
    slots, ids_ref, turned_ref, p_ref, q_ref, left, right, scale, table
):
    members, entries = ids_ref.shape
    cycles_each = entries - slots
    cycles = members * cycles_each
    width = padded(slots * cycles)
    lane = iota((1, width), 1)
    m = jnp.zeros((1, width), jnp.int32)
    for s in range(slots):
        m = jnp.where(lane // cycles == s, ids_ref[0, s], m)
    cycle = jnp.zeros((1, width), jnp.int32)
    for a in range(members):
        for r in range(cycles_each):
            cycle = jnp.where(lane % cycles == a * cycles_each + r, ids_ref[a, slots + r], cycle)
    cosine, sine = angles(cycle.astype(f32))
    legendre_rows(m.astype(f32), cosine, sine, p_ref, q_ref, left, right, scale, table)
    for j in range(width // LANES):
        turned_ref[j * LANES : (j + 1) * LANES] = table[j, :L].T.astype(bf16)


def fourier_kernel(slots, per_slot, ids_ref, fourier_ref):
    members = ids_ref.shape[0]
    every = members * slots
    row = iota((every, 1), 0)
    m_every = jnp.zeros((every, 1), jnp.int32)
    for a in range(members):
        for s in range(slots):
            m_every = jnp.where(row == a * slots + s, ids_ref[a, s], m_every)
    real, imaginary = fourier_rows(m_every)
    is_real = iota((per_slot, NPHI), 0) % 2 == 0
    for j in range(every):
        rows = jnp.where(is_real, real[j : j + 1], imaginary[j : j + 1])
        fourier_ref[j * per_slot : (j + 1) * per_slot] = rows.astype(bf16)


def fourier_stage(ids, slots, per_slot):
    rows = ids.shape[0] * slots * per_slot
    return pl.pallas_call(
        functools.partial(fourier_kernel, slots, per_slot),
        out_shape=jax.ShapeDtypeStruct((rows, NPHI), bf16),
        in_specs=[SMEM],
        out_specs=VMEM,
        compiler_params=pltpu.CompilerParams(vmem_limit_bytes=LIMIT),
        cost_estimate=work(0.5),
        name="fourier_stage",
    )(ids)


def legendre_stage(ids, slots):
    members, entries = ids.shape
    width = padded(slots * members * (entries - slots))
    return pl.pallas_call(
        functools.partial(legendre_kernel, slots),
        out_shape=jax.ShapeDtypeStruct((width, L), bf16),
        in_specs=[SMEM],
        out_specs=VMEM,
        scratch_shapes=[
            pltpu.VMEM((STEPS, BLOCKS, width), f32),
            pltpu.VMEM((STEPS, BLOCKS, width), f32),
            pltpu.VMEM((BLOCKS, width), f32),
            pltpu.VMEM((BLOCKS, width), f32),
            pltpu.VMEM((BLOCKS, width), f32),
            pltpu.VMEM((width // LANES, BLOCKS * STEPS, LANES), f32),
        ],
        compiler_params=pltpu.CompilerParams(vmem_limit_bytes=LIMIT),
        cost_estimate=work(4.0),
        name="legendre_stage",
    )(ids)


def projection_kernel(ids_ref, turned_ref, beam_ref, folded_ref, sums, woven):
    slots, share, _, depth = beam_ref.shape
    cycles = folded_ref.shape[1] // share
    last = L // ROWS
    for pair in range(0, slots, 2):
        low = ids_ref[0, pair] // ROWS
        counts = last - low
        for k in range(last + 1):
            first = (k < counts).astype(jnp.int32)
            slot = pair + 1 - first
            start = jnp.where(k < counts, low + k, last - 1 - low + k - counts)
            start = pl.multiple_of(start * ROWS, ROWS)
            lhs = turned_ref[
                pl.ds(pl.multiple_of(slot * cycles, cycles), cycles), pl.ds(start, ROWS)
            ]
            for c in range(share):
                sums[k, c] = jnp.dot(
                    lhs, beam_ref[slot, c, pl.ds(start, ROWS), :], preferred_element_type=f32
                )
        for s in range(2):
            for c in range(share):
                total = jnp.zeros((cycles, depth), f32)
                for k in range(last + 1):
                    mine = (k < counts) if s == 0 else (k >= counts)
                    total = total + jnp.where(mine, sums[k, c], 0.0)
                for j in range(depth // LANES):
                    woven[s, j, pl.ds(c, cycles, stride=share), :] = total[
                        :, j * LANES : (j + 1) * LANES
                    ]
            for j in range(depth // LANES):
                folded_ref[pair + s, :, j * LANES : (j + 1) * LANES] = woven[s, j].astype(bf16)


def projection(ids, turned, beam, cycles):
    slots, share, _, depth = beam.shape
    return pl.pallas_call(
        projection_kernel,
        out_shape=jax.ShapeDtypeStruct((slots, cycles * share, depth), bf16),
        in_specs=[SMEM, VMEM, VMEM],
        out_specs=VMEM,
        scratch_shapes=[
            pltpu.VMEM((L // ROWS + 1, share, cycles, depth), f32),
            pltpu.VMEM((2, depth // LANES, cycles * share, LANES), f32),
        ],
        compiler_params=pltpu.CompilerParams(vmem_limit_bytes=LIMIT),
        cost_estimate=work(2.0),
        name="projection",
    )(ids, turned, beam)


def cycle_kernel(held_ref, got_ref, folded_ref, *out_refs):
    members = len(out_refs)
    rows, columns = out_refs[0].shape
    slots = folded_ref.shape[0]
    per_member = columns // members
    per_slot = per_member // slots
    share = per_slot // PARTS
    total = held_ref[0] + got_ref[0].astype(f32)
    singular = total.reshape(per_member, total.shape[-1]).astype(bf16)
    singular = jnp.concatenate([singular] * members, axis=0)
    shape = (members * rows, columns)
    row, column = iota(shape, 0), iota(shape, 1)
    slot = (column // per_slot) % slots
    values = jnp.zeros(shape, f32)
    for s in range(slots):
        product = lax.dot_general(
            folded_ref[s], singular, (((1,), (1,)), ((), ())), preferred_element_type=f32
        )
        values = jnp.where(slot == s, product, values)
    same = (row % share == (column // PARTS) % share) & (row // rows == column // per_member)
    values = jnp.where(same, values, 0.0).astype(bf16)
    for a in range(members):
        out_refs[a][...] = values[a * rows : (a + 1) * rows]


def cycle_values(held, got, folded, members):
    _, slots, per_slot, _ = held.shape
    rows = folded.shape[1] // members
    shape = jax.ShapeDtypeStruct((rows, members * slots * per_slot), bf16)
    return pl.pallas_call(
        cycle_kernel,
        out_shape=(shape,) * members,
        in_specs=[VMEM, VMEM, VMEM],
        out_specs=(VMEM,) * members,
        compiler_params=pltpu.CompilerParams(vmem_limit_bytes=LIMIT),
        name="cycle_values",
    )(held, got, folded)


def sky_kernel(members, *refs):
    values_refs, (fourier_ref, out_hbm, maps, sems) = refs[:members], refs[members:]
    rows, columns = values_refs[0].shape
    share = out_hbm.shape[2]
    values = values_refs[0][...].astype(f32)
    for ref in values_refs[1:]:
        values = values + ref[...].astype(f32)
    split = (iota((rows, columns), 1) % PARTS) // 2
    both = jnp.concatenate([jnp.where(split == d, values, 0.0) for d in range(2)], axis=0)
    both = both.astype(bf16)
    width = NPHI // CHUNKS
    copies = []
    for t in range(CHUNKS):
        part = slice(t * width, (t + 1) * width)
        result = jnp.dot(both, fourier_ref[:, part], preferred_element_type=f32)
        for d in range(2):
            maps[:, d, :, part] = result[d * rows : (d + 1) * rows].reshape(
                rows // share, share, width
            )
        copies.append(
            pltpu.make_async_copy(maps.at[:, :, :, part], out_hbm.at[:, :, :, part], sems.at[t])
        )
        copies[-1].start()
    for copy in copies:
        copy.wait()


def sky_maps(values, fourier, share):
    members = len(values)
    shape = (values[0].shape[0] // share, 2, share, NPHI)
    return pl.pallas_call(
        functools.partial(sky_kernel, members),
        out_shape=jax.ShapeDtypeStruct(shape, f32),
        in_specs=[VMEM] * (members + 1),
        out_specs=HBM,
        scratch_shapes=[pltpu.VMEM(shape, f32), pltpu.SemaphoreType.DMA((CHUNKS,))],
        compiler_params=pltpu.CompilerParams(vmem_limit_bytes=LIMIT),
        name="sky_maps",
    )(*values, fourier)


def swap(value, axis, size, bit):
    return lax.ppermute(value, axis, [(k, k ^ bit) for k in range(size)])


def local(members, pieces, m_table, retained_modes, cycle_ids, kl_coeffs, kl_vectors, beam_matrix):
    slots, share = beam_matrix.shape[:2]
    ids = lead(jnp.concatenate([m_table, cycle_ids])[None])
    if members == 4:
        pairs = [
            (a * pieces + k, (a ^ (3 if k % 2 else 1)) * pieces + k)
            for a in range(members)
            for k in range(pieces)
        ]
        first = lax.ppermute(ids, ("ma", "freq"), pairs)
        middle = swap(ids, "ma", members, 2)
        given = swap(first, "freq", pieces, 1)
        ids = gather(ids, first, middle, given)
    else:
        bit = 1
        while bit < members:
            far = swap(ids, "ma", members, bit)
            ids = stack(ids, far)
            bit *= 2
    spread = spread_stage(retained_modes, kl_coeffs, kl_vectors.shape[2])
    held, send = kl_stage(spread, kl_vectors, pieces)
    bit = 1
    while True:
        got = swap(send, "freq", pieces, bit)
        bit *= 2
        if bit == pieces:
            break
        held, send = fold_stage(bit, held, got)
    turned = legendre_stage(ids, slots)
    fourier = fourier_stage(ids, slots, share * PARTS)
    folded = projection(ids, turned, beam_matrix, members * cycle_ids.shape[0])
    values = cycle_values(held, got, folded, members)
    gathered = [values[0]]
    for j in range(1, members):
        gathered.append(swap(values[j], "ma", members, j))
    values = gathered
    return sky_maps(values, fourier, share)


def solution(mesh):
    placed = (
        P("ma"),
        P("ma"),
        P("ma"),
        P("ma", None, "freq"),
        P("ma", "freq", None, None),
        P("ma", "freq", None, None),
    )
    return jax.shard_map(
        functools.partial(local, mesh.shape["ma"], mesh.shape["freq"]),
        mesh=mesh,
        in_specs=placed,
        out_specs=P("ma", None, "freq", None),
        check_vma=False,
    )
```

```python
import functools
import math

import jax
import jax.numpy as jnp
from jax import lax
from jax.experimental import pallas as pl
from jax.experimental.pallas import tpu as pltpu
from jax.sharding import PartitionSpec as P


NPHI = 2048
L = 1024
NSIDE = 512
PARTS = 4
BLOCKS = 32
STEPS = L // BLOCKS + 1
ROWS = 256
LANES = 128
CHUNKS = 4
GROUP = 16


f32 = jnp.float32
bf16 = jnp.bfloat16
VMEM = pl.BlockSpec(memory_space=pltpu.VMEM)
SMEM = pl.BlockSpec(memory_space=pltpu.SMEM)
HBM = pl.BlockSpec(memory_space=pltpu.HBM)
LIMIT = 16 * 1024 * 1024
SMALL = 2 * 1024 * 1024


def padded(width):
    return -(-width // LANES) * LANES


def iota(shape, axis):
    return lax.broadcasted_iota(jnp.int32, shape, axis)


def work(microseconds):
    return pl.CostEstimate(
        flops=int(microseconds * 1e9), transcendentals=0, bytes_accessed=4096
    )


def lead_kernel(in_ref, out_ref):
    out_ref[...] = in_ref[...]


def lead(ids):
    return pl.pallas_call(
        lead_kernel,
        out_shape=jax.ShapeDtypeStruct(ids.shape, ids.dtype),
        in_specs=[VMEM],
        out_specs=VMEM,
        compiler_params=pltpu.CompilerParams(vmem_limit_bytes=SMALL),
        cost_estimate=work(3.0),
        name="lead",
    )(ids)


def spread_kernel(kept_ref, coeff_ref, out_ref):
    slots, rows, columns = out_ref.shape
    modes = coeff_ref.shape[2]
    group = columns // modes
    place = lax.axis_index("freq")
    expand = (iota((modes, columns), 1) // group == iota((modes, columns), 0)).astype(bf16)
    mode_index = place * modes + iota((PARTS, modes), 1)
    tall = []
    for s in range(slots):
        kept = mode_index < kept_ref[:, s : s + 1]
        tall += [jnp.where(kept, coeff_ref[s].astype(f32), 0.0)] * 2
    wide = jnp.dot(
        jnp.concatenate(tall, axis=0).astype(bf16), expand, preferred_element_type=f32
    )
    period = max(group, LANES)
    diagonal = iota((rows, period), 1) % group == iota((rows, period), 0) // PARTS
    for s in range(slots):
        for t in range(columns // period):
            lanes = slice(t * period, (t + 1) * period)
            piece = wide[s * 2 * PARTS : (s + 1) * 2 * PARTS, lanes]
            piece = jnp.concatenate([piece] * (rows // (2 * PARTS)), axis=0)
            out_ref[s, :, lanes] = jnp.where(diagonal, piece, 0.0).astype(bf16)


def spread_stage(kept, coeffs, channels):
    slots, _, modes = coeffs.shape
    group = min(GROUP, channels)
    return pl.pallas_call(
        spread_kernel,
        out_shape=jax.ShapeDtypeStruct((slots, group * PARTS, modes * group), bf16),
        in_specs=[VMEM, VMEM],
        out_specs=VMEM,
        compiler_params=pltpu.CompilerParams(vmem_limit_bytes=SMALL),
        cost_estimate=work(0.5),
        name="spread_stage",
    )(kept[None], coeffs)


def kl_kernel(spread_ref, vectors_ref, keep_ref, send_ref):
    slots, modes, channels, depth = vectors_ref.shape
    group = spread_ref.shape[1] // PARTS
    pieces = keep_ref.shape[0] * 2
    share = channels // pieces
    rows = share * PARTS
    even = lax.axis_index("freq") % 2 == 0
    for s in range(slots):
        for g in range(channels // group):
            block = vectors_ref[s, :, g * group : (g + 1) * group, :]
            sums = jnp.dot(
                spread_ref[s], block.reshape(modes * group, depth), preferred_element_type=f32
            )
            for i in range(group // share // 2):
                pair = g * (group // share // 2) + i
                first = sums[2 * i * rows : (2 * i + 1) * rows]
                second = sums[(2 * i + 1) * rows : (2 * i + 2) * rows]
                keep_ref[pair, s] = jnp.where(even, first, second)
                send_ref[pair, s] = jnp.where(even, second, first).astype(bf16)


def kl_stage(spread, vectors, pieces):
    slots, _, channels, depth = vectors.shape
    shape = (pieces // 2, slots, channels // pieces * PARTS, depth)
    return pl.pallas_call(
        kl_kernel,
        out_shape=(jax.ShapeDtypeStruct(shape, f32), jax.ShapeDtypeStruct(shape, bf16)),
        in_specs=[VMEM, VMEM],
        out_specs=(VMEM, VMEM),
        compiler_params=pltpu.CompilerParams(vmem_limit_bytes=LIMIT),
        cost_estimate=work(2.0),
        name="kl_stage",
    )(spread, vectors)


def gather_kernel(own_ref, first_ref, middle_ref, given_ref, out_ref):
    odd = lax.axis_index("freq") % 2 == 1
    first, given = first_ref[...], given_ref[...]
    out_ref[0:1] = own_ref[...]
    out_ref[1:2] = jnp.where(odd, given, first)
    out_ref[2:3] = middle_ref[...]
    out_ref[3:4] = jnp.where(odd, first, given)


def gather(*rows):
    return pl.pallas_call(
        gather_kernel,
        out_shape=jax.ShapeDtypeStruct((4, rows[0].shape[1]), rows[0].dtype),
        in_specs=[VMEM] * 4,
        out_specs=VMEM,
        compiler_params=pltpu.CompilerParams(vmem_limit_bytes=SMALL),
        name="gather",
    )(*rows)


def fold_kernel(bit, held_ref, got_ref, keep_ref, send_ref):
    mine = (lax.axis_index("freq") // bit) % 2
    for i in range(keep_ref.shape[0]):
        keep_ref[i] = held_ref[2 * i + mine] + got_ref[2 * i + mine].astype(f32)
        other = 2 * i + 1 - mine
        send_ref[i] = (held_ref[other] + got_ref[other].astype(f32)).astype(bf16)


def fold_stage(bit, held, got):
    shape = (held.shape[0] // 2, *held.shape[1:])
    return pl.pallas_call(
        functools.partial(fold_kernel, bit),
        out_shape=(jax.ShapeDtypeStruct(shape, f32), jax.ShapeDtypeStruct(shape, bf16)),
        in_specs=[VMEM, VMEM],
        out_specs=(VMEM, VMEM),
        compiler_params=pltpu.CompilerParams(vmem_limit_bytes=LIMIT),
        name="fold_stage",
    )(held, got)


def stack_kernel(low_ref, high_ref, out_ref):
    rows = low_ref.shape[0]
    out_ref[:rows] = low_ref[...]
    out_ref[rows:] = high_ref[...]


def stack(low, high):
    return pl.pallas_call(
        stack_kernel,
        out_shape=jax.ShapeDtypeStruct((2 * low.shape[0], low.shape[1]), low.dtype),
        in_specs=[VMEM, VMEM],
        out_specs=VMEM,
        compiler_params=pltpu.CompilerParams(vmem_limit_bytes=SMALL),
        name="stack",
    )(low, high)


def angles(cycle):
    n = float(NSIDE)
    p = jnp.minimum(cycle, 4.0 * n - cycle)
    t = p * p / (3.0 * n * n)
    cap_sin = p * (1.0 / (math.sqrt(3.0) * n)) * jnp.sqrt(2.0 - t)
    belt_cos = 4.0 / 3.0 - p * (2.0 / (3.0 * n))
    belt_sin = jnp.sqrt(jnp.maximum(1.0 - belt_cos * belt_cos, 0.25))
    cap = p < n
    cosine = jnp.where(cap, 1.0 - t, belt_cos)
    return jnp.where(cycle <= 2.0 * n, cosine, -cosine), jnp.where(cap, cap_sin, belt_sin)


def log2_start(m, sine):
    x = m + 4.25
    y = 1.0 / (x * x)
    series = 1.0 + y * (-1.0 / 64.0 + y * (21.0 / 8192.0 - y * (671.0 / 524288.0)))
    product = series * lax.rsqrt(x) * (1.0 / math.sqrt(math.pi))
    for k in range(1, 5):
        product = product * ((m + k) / (m + (k - 0.5)))
    scale = (2.0 * m + 1.0) * (1.0 / (4.0 * math.pi)) * product
    return (0.5 * jnp.log(scale) + m * jnp.log(sine)) * (1.0 / math.log(2.0))


def legendre_rows(m, cosine, sine, p_ref, q_ref, left, right, scale, table):
    width = m.shape[1]
    first = (iota((BLOCKS, width), 0) * STEPS).astype(f32)
    m_all = jnp.broadcast_to(m, (BLOCKS, width))
    c_all = jnp.broadcast_to(cosine, (BLOCKS, width))
    began = first > m_all
    p1 = jnp.where(began, 1.0, 0.0)
    p0 = jnp.zeros_like(p1)
    q1 = jnp.zeros_like(p1)
    q0 = p1

    def factors(l):
        over = (l - m_all) * (l + m_all)
        under = 4.0 * l * l - 1.0
        root = lax.rsqrt(jnp.maximum(over, 1.0) * jnp.maximum(under, 1.0))
        live = over > 0.0
        return jnp.where(live, under * root, 0.0), jnp.where(live, over * root, 0.0)

    _, last_inverse = factors(first - 1.0)
    last_inverse = jnp.where(began, last_inverse, 0.0)
    for i in range(STEPS):
        l = first + float(i)
        a, inverse = factors(l)
        above = l > m_all
        a = jnp.where(above, a, 0.0)
        rise = a * c_all
        fall = a * last_inverse
        p2 = rise * p1 - fall * p0
        q2 = rise * q1 - fall * q0
        p2 = jnp.where(l == m_all, 1.0, p2)
        p1, p0 = p2, p1
        q1, q0 = q2, q1
        last_inverse = jnp.where(above, inverse, 0.0)
        p_ref[i] = p2
        q_ref[i] = q2

    size = jnp.maximum(
        jnp.maximum(jnp.abs(p1), jnp.abs(p0)), jnp.maximum(jnp.abs(q1), jnp.abs(q0))
    )
    power = jnp.floor(jnp.log(jnp.maximum(size, 1.0)) * (1.0 / math.log(2.0)))
    power = jnp.where(power >= 20.0, power, 0.0)
    shrink = jnp.exp2(-power)
    p1, p0, q1, q0 = p1 * shrink, p0 * shrink, q1 * shrink, q0 * shrink

    start = log2_start(m, sine)
    start_power = jnp.floor(start)
    start_value = jnp.exp2(start - start_power)
    here = jnp.zeros((1, width), f32)
    before = jnp.zeros((1, width), f32)
    level = jnp.zeros((1, width), f32)
    for b in range(BLOCKS):
        enters = (m >= float(b * STEPS)) & (m < float((b + 1) * STEPS))
        here = jnp.where(enters, start_value, here)
        before = jnp.where(enters, 0.0, before)
        level = jnp.where(enters, start_power, level)
        left[b : b + 1] = here
        right[b : b + 1] = before
        scale[b : b + 1] = level
        here, before = (
            p1[b : b + 1] * here + q1[b : b + 1] * before,
            p0[b : b + 1] * here + q0[b : b + 1] * before,
        )
        large = jnp.maximum(jnp.abs(here), jnp.abs(before)) > 2.0**30
        factor = jnp.where(large, 2.0**-30, 1.0)
        here = here * factor
        before = before * factor
        level = level + power[b : b + 1] + jnp.where(large, 30.0, 0.0)

    half = jnp.exp2(jnp.maximum(scale[...] * 0.5, -120.0))
    from_left = left[...] * half
    from_right = right[...] * half
    for i in range(STEPS):
        rows = (from_left * p_ref[i] + from_right * q_ref[i]) * half
        for j in range(width // LANES):
            table[j, pl.ds(i, BLOCKS, stride=STEPS), :] = rows[:, j * LANES : (j + 1) * LANES]


def sine_quarter(z):
    x = z * (2.0 * math.pi)
    y = x * x
    return x * (
        1.0
        + y
        * (
            -1.0 / 6.0
            + y * (1.0 / 120.0 + y * (-1.0 / 5040.0 + y * (1.0 / 362880.0 - y / 39916800.0)))
        )
    )


def fourier_rows(m):
    turn = (m * iota((m.shape[0], NPHI), 1)) % NPHI
    z = turn.astype(f32) * (1.0 / NPHI)
    z = jnp.where(z >= 0.5, z - 1.0, z)
    size = jnp.abs(z)
    cosine = sine_quarter(0.25 - size)
    folded = sine_quarter(jnp.where(size > 0.25, 0.5 - size, size))
    sine = jnp.where(z < 0.0, -folded, folded)
    weight = jnp.where(m == 0, 1.0, 2.0)
    return weight * cosine, -weight * sine


def legendre_kernel(
    slots, ids_ref, turned_ref, p_ref, q_ref, left, right, scale, table
):
    members, entries = ids_ref.shape
    cycles_each = entries - slots
    cycles = members * cycles_each
    width = padded(slots * cycles)
    lane = iota((1, width), 1)
    m = jnp.zeros((1, width), jnp.int32)
    for s in range(slots):
        m = jnp.where(lane // cycles == s, ids_ref[0, s], m)
    cycle = jnp.zeros((1, width), jnp.int32)
    for a in range(members):
        for r in range(cycles_each):
            cycle = jnp.where(lane % cycles == a * cycles_each + r, ids_ref[a, slots + r], cycle)
    cosine, sine = angles(cycle.astype(f32))
    legendre_rows(m.astype(f32), cosine, sine, p_ref, q_ref, left, right, scale, table)
    for j in range(width // LANES):
        turned_ref[j * LANES : (j + 1) * LANES] = table[j, :L].T.astype(bf16)


def fourier_kernel(slots, per_slot, ids_ref, fourier_ref):
    members = ids_ref.shape[0]
    every = members * slots
    row = iota((every, 1), 0)
    m_every = jnp.zeros((every, 1), jnp.int32)
    for a in range(members):
        for s in range(slots):
            m_every = jnp.where(row == a * slots + s, ids_ref[a, s], m_every)
    real, imaginary = fourier_rows(m_every)
    is_real = iota((per_slot, NPHI), 0) % 2 == 0
    for j in range(every):
        rows = jnp.where(is_real, real[j : j + 1], imaginary[j : j + 1])
        fourier_ref[j * per_slot : (j + 1) * per_slot] = rows.astype(bf16)


def fourier_stage(ids, slots, per_slot):
    rows = ids.shape[0] * slots * per_slot
    return pl.pallas_call(
        functools.partial(fourier_kernel, slots, per_slot),
        out_shape=jax.ShapeDtypeStruct((rows, NPHI), bf16),
        in_specs=[SMEM],
        out_specs=VMEM,
        compiler_params=pltpu.CompilerParams(vmem_limit_bytes=LIMIT),
        cost_estimate=work(0.5),
        name="fourier_stage",
    )(ids)


def legendre_stage(ids, slots):
    members, entries = ids.shape
    width = padded(slots * members * (entries - slots))
    return pl.pallas_call(
        functools.partial(legendre_kernel, slots),
        out_shape=jax.ShapeDtypeStruct((width, L), bf16),
        in_specs=[SMEM],
        out_specs=VMEM,
        scratch_shapes=[
            pltpu.VMEM((STEPS, BLOCKS, width), f32),
            pltpu.VMEM((STEPS, BLOCKS, width), f32),
            pltpu.VMEM((BLOCKS, width), f32),
            pltpu.VMEM((BLOCKS, width), f32),
            pltpu.VMEM((BLOCKS, width), f32),
            pltpu.VMEM((width // LANES, BLOCKS * STEPS, LANES), f32),
        ],
        compiler_params=pltpu.CompilerParams(vmem_limit_bytes=LIMIT),
        cost_estimate=work(4.0),
        name="legendre_stage",
    )(ids)


def projection_kernel(ids_ref, turned_ref, beam_ref, folded_ref, sums, woven):
    slots, share, _, depth = beam_ref.shape
    cycles = folded_ref.shape[1] // share
    last = L // ROWS
    for pair in range(0, slots, 2):
        low = ids_ref[0, pair] // ROWS
        counts = last - low
        for k in range(last + 1):
            first = (k < counts).astype(jnp.int32)
            slot = pair + 1 - first
            start = jnp.where(k < counts, low + k, last - 1 - low + k - counts)
            start = pl.multiple_of(start * ROWS, ROWS)
            lhs = turned_ref[
                pl.ds(pl.multiple_of(slot * cycles, cycles), cycles), pl.ds(start, ROWS)
            ]
            for c in range(share):
                sums[k, c] = jnp.dot(
                    lhs, beam_ref[slot, c, pl.ds(start, ROWS), :], preferred_element_type=f32
                )
        for s in range(2):
            for c in range(share):
                total = jnp.zeros((cycles, depth), f32)
                for k in range(last + 1):
                    mine = (k < counts) if s == 0 else (k >= counts)
                    total = total + jnp.where(mine, sums[k, c], 0.0)
                for j in range(depth // LANES):
                    woven[s, j, pl.ds(c, cycles, stride=share), :] = total[
                        :, j * LANES : (j + 1) * LANES
                    ]
            for j in range(depth // LANES):
                folded_ref[pair + s, :, j * LANES : (j + 1) * LANES] = woven[s, j].astype(bf16)


def projection(ids, turned, beam, cycles):
    slots, share, _, depth = beam.shape
    return pl.pallas_call(
        projection_kernel,
        out_shape=jax.ShapeDtypeStruct((slots, cycles * share, depth), bf16),
        in_specs=[SMEM, VMEM, VMEM],
        out_specs=VMEM,
        scratch_shapes=[
            pltpu.VMEM((L // ROWS + 1, share, cycles, depth), f32),
            pltpu.VMEM((2, depth // LANES, cycles * share, LANES), f32),
        ],
        compiler_params=pltpu.CompilerParams(vmem_limit_bytes=LIMIT),
        cost_estimate=work(2.0),
        name="projection",
    )(ids, turned, beam)


def cycle_kernel(held_ref, got_ref, folded_ref, *out_refs):
    members = len(out_refs)
    rows, columns = out_refs[0].shape
    slots = folded_ref.shape[0]
    per_member = columns // members
    per_slot = per_member // slots
    share = per_slot // PARTS
    total = held_ref[0] + got_ref[0].astype(f32)
    singular = total.reshape(per_member, total.shape[-1]).astype(bf16)
    singular = jnp.concatenate([singular] * members, axis=0)
    shape = (members * rows, columns)
    row, column = iota(shape, 0), iota(shape, 1)
    slot = (column // per_slot) % slots
    values = jnp.zeros(shape, f32)
    for s in range(slots):
        product = lax.dot_general(
            folded_ref[s], singular, (((1,), (1,)), ((), ())), preferred_element_type=f32
        )
        values = jnp.where(slot == s, product, values)
    same = (row % share == (column // PARTS) % share) & (row // rows == column // per_member)
    values = jnp.where(same, values, 0.0).astype(bf16)
    for a in range(members):
        out_refs[a][...] = values[a * rows : (a + 1) * rows]


def cycle_values(held, got, folded, members):
    _, slots, per_slot, _ = held.shape
    rows = folded.shape[1] // members
    shape = jax.ShapeDtypeStruct((rows, members * slots * per_slot), bf16)
    return pl.pallas_call(
        cycle_kernel,
        out_shape=(shape,) * members,
        in_specs=[VMEM, VMEM, VMEM],
        out_specs=(VMEM,) * members,
        compiler_params=pltpu.CompilerParams(vmem_limit_bytes=LIMIT),
        name="cycle_values",
    )(held, got, folded)


def sky_kernel(members, *refs):
    values_refs, (fourier_ref, out_hbm, maps, sems) = refs[:members], refs[members:]
    rows, columns = values_refs[0].shape
    share = out_hbm.shape[2]
    values = values_refs[0][...].astype(f32)
    for ref in values_refs[1:]:
        values = values + ref[...].astype(f32)
    split = (iota((rows, columns), 1) % PARTS) // 2
    both = jnp.concatenate([jnp.where(split == d, values, 0.0) for d in range(2)], axis=0)
    both = both.astype(bf16)
    width = NPHI // CHUNKS
    copies = []
    for t in range(CHUNKS):
        part = slice(t * width, (t + 1) * width)
        result = jnp.dot(both, fourier_ref[:, part], preferred_element_type=f32)
        for d in range(2):
            maps[:, d, :, part] = result[d * rows : (d + 1) * rows].reshape(
                rows // share, share, width
            )
        copies.append(
            pltpu.make_async_copy(maps.at[:, :, :, part], out_hbm.at[:, :, :, part], sems.at[t])
        )
        copies[-1].start()
    for copy in copies:
        copy.wait()


def sky_maps(values, fourier, share):
    members = len(values)
    shape = (values[0].shape[0] // share, 2, share, NPHI)
    return pl.pallas_call(
        functools.partial(sky_kernel, members),
        out_shape=jax.ShapeDtypeStruct(shape, f32),
        in_specs=[VMEM] * (members + 1),
        out_specs=HBM,
        scratch_shapes=[pltpu.VMEM(shape, f32), pltpu.SemaphoreType.DMA((CHUNKS,))],
        compiler_params=pltpu.CompilerParams(vmem_limit_bytes=LIMIT),
        name="sky_maps",
    )(*values, fourier)


def swap(value, axis, size, bit):
    return lax.ppermute(value, axis, [(k, k ^ bit) for k in range(size)])


def local(members, pieces, m_table, retained_modes, cycle_ids, kl_coeffs, kl_vectors, beam_matrix):
    slots, share = beam_matrix.shape[:2]
    ids = lead(jnp.concatenate([m_table, cycle_ids])[None])
    if members == 4:
        pairs = [
            (a * pieces + k, (a ^ (3 if k % 2 else 1)) * pieces + k)
            for a in range(members)
            for k in range(pieces)
        ]
        first = lax.ppermute(ids, ("ma", "freq"), pairs)
        middle = swap(ids, "ma", members, 2)
        given = swap(first, "freq", pieces, 1)
        ids = gather(ids, first, middle, given)
    else:
        bit = 1
        while bit < members:
            far = swap(ids, "ma", members, bit)
            ids = stack(ids, far)
            bit *= 2
    spread = spread_stage(retained_modes, kl_coeffs, kl_vectors.shape[2])
    held, send = kl_stage(spread, kl_vectors, pieces)
    bit = 1
    while True:
        got = swap(send, "freq", pieces, bit)
        bit *= 2
        if bit == pieces:
            break
        held, send = fold_stage(bit, held, got)
    turned = legendre_stage(ids, slots)
    fourier = fourier_stage(ids, slots, share * PARTS)
    folded = projection(ids, turned, beam_matrix, members * cycle_ids.shape[0])
    values = cycle_values(held, got, folded, members)
    gathered = [values[0]]
    for j in range(1, members):
        gathered.append(swap(values[j], "ma", members, j))
    values = gathered
    return sky_maps(values, fourier, share)


def solution(mesh):
    placed = (
        P("ma"),
        P("ma"),
        P("ma"),
        P("ma", None, "freq"),
        P("ma", "freq", None, None),
        P("ma", "freq", None, None),
    )
    return jax.shard_map(
        functools.partial(local, mesh.shape["ma"], mesh.shape["freq"]),
        mesh=mesh,
        in_specs=placed,
        out_specs=P("ma", None, "freq", None),
        check_vma=False,
    )
```
